128 devices in a mesh: px: 8 (over z_hi, y), py: 16 (over x, z_lo, core).
Axes of the slice: x: 4, y: 4, z: 4 (z_hi: 2, z_lo: 2; z = z_hi * 2 + z_lo), core: 2. Of those that a mesh axis runs over, the one named last changes fastest.
Arguments:
- white_noise: float32 [2, 128, 512, 256], P(None, 'px', 'py'), may hold values from -6 to 6
- spectrum: float32 [128, 512, 256], P('px', 'py'), may hold values from 0.1 to 2, as said below
- group_table: int32 [3, 16], replicated, may hold values from 0 to 15, each once within a row
Outputs:
- modulus: float32 [2, 128, 512, 256], P(None, 'px', 'py')
- level_one: float32 [2, 64, 256, 128], P(None, 'px', 'py')
- level_two: float32 [2, 32, 128, 64], P(None, 'px', 'py')
- level_three: float32 [2, 16, 64, 32], P(None, 'px', 'py')
The draws below stay inside these ranges and needn't reach their ends.
Inputs may be any that keep to these rules, and one draw needn't show every extreme that they name: spectrum[j, m, k] equals spectrum[(128 - j) % 128, (512 - m) % 512, (256 - k) % 256]. `group_table`: each row is a permutation of 0 to 15.
All inputs are finite; a program needn't handle non-finite values.
Results may differ from the reference program's by a relative error of at most 0.000088.
Values sent between devices are 32-bit elements; how exact they have to be, the bound alone decides.
A program may use at most 192 MiB of HBM per device.

```python
import math
import jax
import jax.numpy as jnp

FIELDS = 2
LEVELS = 3
NZ = 256
NX = 128
NY = 512
N_PY = 16


def draw_spectrum(key, part):
    log_low = math.log(0.1)
    log_high = math.log(2.0)
    rough_part = jnp.exp(jax.random.uniform(key, (NX, NY, NZ), jnp.float32, log_low, log_high))
    mirror = jnp.roll(jnp.flip(rough_part, (0, 1, 2)), 1, (0, 1, 2))
    values = 0.5 * (rough_part + mirror)
    return values


def level_of(stream_key, extent, shards, low, top_value):
    def one(axis_at, blocks):
        draws = jax.random.uniform(jax.random.fold_in(jax.random.fold_in(stream_key, 6), axis_at), (blocks,), jnp.float32, low / len(shards), top_value / len(shards))
        return jnp.repeat(jnp.exp(draws), extent[axis_at] // blocks).reshape((-1,) + (1,) * (len(extent) - axis_at - 1))

    level = one(*shards[0])
    for cut in shards[1:]:
        level = level * one(*cut)
    return level


def normal_values(own_key, shape, deviation, most, split=(), dtype=jnp.bfloat16):
    array = jax.random.normal(own_key, shape, jnp.float32) * deviation
    if len(split) > 0:
        array = level_of(own_key, shape, split, -0.22, 0.18) * array
    return jnp.clip(array, min=-most, max=most).astype(dtype)


def setup_inputs(seed: int = 0) -> dict:
    arg_keys = jax.random.split(jax.random.key(seed), 4)
    white_noise = normal_values(arg_keys[0], (FIELDS, NX, NY, NZ), 1.0, 6.0, ((1, 8), (2, 16)), jnp.float32)
    spectrum = draw_spectrum(jax.random.fold_in(arg_keys[3], 71), 0)
    group_table = jax.vmap(lambda own: jax.random.permutation(own, N_PY))(jax.random.split(arg_keys[2], LEVELS)).reshape((LEVELS, N_PY)).astype(jnp.int32)
    return dict(white_noise=white_noise, spectrum=spectrum, group_table=group_table)


def coarsen(values):
    members, size_x, size_y, size_z = values.shape
    blocks = values.reshape(members, size_x // 2, 2, size_y // 2, 2, size_z // 2, 2)
    return blocks.mean(axis=(2, 4, 6))


def route_blocks(coarse, group_order):
    members, size_x, size_y, size_z = coarse.shape
    blocks = coarse.reshape(members, size_x, N_PY, size_y // N_PY, size_z)
    picked = jnp.take(blocks, group_order, axis=2)
    return picked.reshape(members, size_x, size_y, size_z)


def reference(white_noise, spectrum, group_table):
    spectra = jnp.fft.fftn(white_noise, axes=(1, 2, 3))
    scaled = spectra * spectrum[None]
    fields_real = jnp.real(jnp.fft.ifftn(scaled, axes=(1, 2, 3)))
    modulus = jnp.exp(0.5 * fields_real)
    coarse_one = coarsen(modulus)
    coarse_two = coarsen(coarse_one)
    coarse_three = coarsen(coarse_two)
    level_one = route_blocks(coarse_one, group_table[0])
    level_two = route_blocks(coarse_two, group_table[1])
    level_three = route_blocks(coarse_three, group_table[2])
    return modulus, level_one, level_two, level_three
```

```python
import functools

import jax
import jax.numpy as jnp
import ml_dtypes
import numpy as np
from jax import lax
from jax.experimental import pallas as pl
from jax.experimental.pallas import tpu as pltpu
from jax.sharding import Mesh
from jax.sharding import PartitionSpec as P

PX = ("px_0", "px_1")
PY = ("py_0", "py_1", "py_2")
F32 = jnp.float32
BF16 = jnp.bfloat16
LOGICAL = pl.DeviceIdType.LOGICAL

NX, NY, NZ = 128, 512, 256
CX, CY = 16, 32
CELLS = CX * CY
T_Z, T_P, T_C, T_CI, T_PI, T_U, TABLES = 0, 1, 2, 6, 10, 11, 12
PIECE = 24


def wave(products, length, sign):
    angles = 2.0 * np.pi * (products % length) / length
    return np.cos(angles), sign * np.sin(angles)


def applied_left(real, imag):
    return np.block([[real, -imag], [imag, real]])


def build_tables():
    spots = np.arange(128)
    z = np.arange(NZ)
    p, q = spots // 16, spots % 16
    j1, m1 = spots // 16, spots % 16
    tables = np.zeros((TABLES, 256, 256))
    cos_z, sin_z = wave(spots[:, None] * z[None, :], NZ, -1.0)
    sin_z[0] = (-1.0) ** z
    tables[T_Z] = np.concatenate([cos_z, sin_z], 0)
    weight = np.where(spots == 0, 1.0, 2.0)[:, None] / float(NX * NY * NZ)
    tables[T_U] = np.concatenate([cos_z * weight, sin_z * weight], 0)
    outer = 2 * p[None, :] * j1[:, None] + q[None, :] * m1[:, None]
    tables[T_P] = applied_left(*wave(outer, 16, -1.0))
    tables[T_PI] = applied_left(*wave(outer.T, 16, 1.0))
    low, b = spots // 32, spots % 32
    half, j2b, q2 = spots // 64, (spots // 16) % 4, spots % 16
    m2 = 2 * q2 + half
    for j2a in range(4):
        inner = 2 * low[:, None] * j2a + 8 * low[:, None] * j2b[None, :] + b[:, None] * m2[None, :]
        tables[T_C + j2a] = applied_left(*wave(inner.T, 32, -1.0)).T
        tables[T_CI + j2a] = applied_left(*wave(inner, 32, 1.0)).T
    cell_a, cell_b = np.arange(CELLS) // CY, np.arange(CELLS) % CY
    middle = 4 * cell_a[None, :] * j1[:, None] + cell_b[None, :] * m1[:, None]
    twiddle = np.stack(wave(middle, 512, -1.0)).astype(np.float32)
    high = tables.astype(np.float32).astype(ml_dtypes.bfloat16)
    rest = (tables - high.astype(np.float64)).astype(np.float32).astype(ml_dtypes.bfloat16)
    pairs = np.zeros((NZ, 256))
    pairs[z, z // 2] = 0.5
    pairs[z, 128 + z // 4] = 0.25
    pairs[z, 192 + z // 8] = 0.125
    rows = np.zeros((8 * PIECE, CELLS))
    for cell in range(CELLS):
        a, b = divmod(cell, CY)
        rows[(a // 2) * PIECE + b // 2, cell] = 0.25
        second = (a // 4) * 8 + b // 4
        rows[(second // 4) * PIECE + 16 + second % 4, cell] = 1.0 / 16
        third = (a // 8) * 4 + b // 8
        rows[third * PIECE + 20, cell] = 1.0 / 64
    exact = ml_dtypes.bfloat16
    return np.stack([high, rest], 1), twiddle, pairs.astype(exact), rows.astype(exact)


def dot(left, right):
    return jnp.dot(left, right, preferred_element_type=F32)


def dot_nt(left, right):
    return lax.dot_general(left, right, (((1,), (1,)), ((), ())), preferred_element_type=F32)


def split(values):
    high = values.astype(BF16)
    return high, (values - high.astype(F32)).astype(BF16)


def ordered(index):
    return lax.rem(2 - index + 3 * (index // 2) + 2 * (index // 3) + 4, 4)


def kernel(
    noise_hbm, spec_hbm, order_ref, tables_hbm, twiddle_hbm, pairs_hbm, rows_hbm,
    modulus_ref, one_ref, two_ref, three_ref,
    noise, spec, tables, twiddle, pairs, rows,
    s_send, s_recv, n_send, scale, f_send, f_recv, b_send, b_recv,
    y_mid, v_high, v_low, v_back, z_high, z_low, g_high, g_low,
    r_send, r_recv, t_send, t_recv,
    load_sems, send_sems, recv_sems,
):
    zh, y, x, zl, c = [lax.axis_index(a) for a in (*PX, *PY)]
    z = zh * 2 + zl
    line = zh * 64 + y * 16
    column = x * 4 + zl * 2 + c
    me = line + column

    loads = []
    for k, (source, target) in enumerate((
        (spec_hbm, spec), (tables_hbm.at[T_Z], tables.at[T_Z]), (noise_hbm, noise),
        (tables_hbm.at[pl.ds(1, TABLES - 1)], tables.at[pl.ds(1, TABLES - 1)]),
        (twiddle_hbm, twiddle), (pairs_hbm, pairs), (rows_hbm, rows),
    )):
        load = pltpu.make_async_copy(source, target, load_sems.at[k])
        load.start()
        loads.append(load)

    def over_devices(action):
        def group(n, skip):
            core = lax.rem(c + 1 - n // 4, 2)
            s = lax.rem(n, 4)
            z2 = lax.rem(z + ordered(s), 4)
            base = (z2 // 2) * 64 + lax.rem(z2, 2) * 2 + core
            ys = [base + lax.rem(y + ordered(lax.rem(s + t, 4)), 4) * 16 for t in range(4)]
            xs = [lax.rem(x + ordered(lax.rem(s + t, 4)), 4) * 4 for t in range(4)]
            for t in range(4):
                for u in range(4):
                    if not (skip and t == 0 and u == 0):
                        action(ys[t] + xs[u])

        @pl.loop(0, 7)
        def _(n):
            group(n, False)

        group(jnp.int32(7), True)

    barrier = pltpu.get_barrier_semaphore()
    over_devices(lambda d: pl.semaphore_signal(barrier, 1, device_id=d, device_id_type=LOGICAL))

    def send_all(source, target, index):
        over_devices(lambda d: pltpu.make_async_remote_copy(
            source(d), target(me), send_sems.at[index], recv_sems.at[index],
            device_id=d, device_id_type=LOGICAL).start())

    def finish(ref, sem):
        pltpu.make_async_copy(ref, ref, sem).wait()

    loads[0].wait()
    for jj in range(4):
        j2lo, m2lo = divmod(jj, 2)
        starts = [(j2lo * 8 + j1) * CY + m2lo * 16 for j1 in range(8)]
        block = jnp.concatenate([spec[pl.ds(s, 16), 0:128] for s in starts], 0)
        s_send[:, jj, :] = block.T
        block = jnp.concatenate([spec[pl.ds(s, 16), 128:256] for s in starts], 0)
        n_send[0, jj, :] = block.T[0]

    pl.semaphore_wait(barrier, 127)
    send_all(lambda d: s_send.at[d], lambda m: s_recv.at[0, m], 0)
    s_recv[0, me] = s_send[me]

    @pl.when(me != 0)
    def _():
        pltpu.make_async_remote_copy(
            n_send.at[0], s_recv.at[1, me], send_sems.at[1], recv_sems.at[1],
            device_id=jnp.int32(0), device_id_type=LOGICAL).start()

    @pl.when(me == 0)
    def _():
        s_recv[1, 0] = n_send[0]

    loads[1].wait()
    loads[2].wait()

    @pl.loop(0, 2)
    def _(f):
        for part in range(2):
            high, low = split(noise[f, pl.ds(part * 256, 256), :])
            out = dot_nt(tables[T_Z, 0], high) + dot_nt(tables[T_Z, 0], low) + dot_nt(tables[T_Z, 1], high)
            for ri in range(2):
                for l in range(2):
                    f_send[f, pl.ds(ri * 4 + part * 2 + l, 128, stride=8), :] = (
                        out[ri * 128:(ri + 1) * 128, l * 128:(l + 1) * 128])

    def swap_first(ref):
        first, second = ref[0, pl.ds(0, 8), :], ref[1, pl.ds(0, 8), :]
        ref[0, pl.ds(0, 8), :] = jnp.concatenate([first[:4], second[:4]], 0)
        ref[1, pl.ds(0, 8), :] = jnp.concatenate([first[4:], second[4:]], 0)

    def block_of(d):
        return pl.ds(pl.multiple_of(d * 8, 8), 8)

    swap_first(f_send)

    @pl.loop(0, 2)
    def _(f):
        send_all(lambda d: f_send.at[f, block_of(d)], lambda m: f_recv.at[f, block_of(m)], 2 + f)
        f_recv[f, block_of(me), :] = f_send[f, block_of(me), :]

    finish(s_recv.at[0, pl.ds(0, 127)], recv_sems.at[0])

    @pl.when(me == 0)
    def _():
        finish(s_recv.at[0, pl.ds(0, 127)], recv_sems.at[1])

    for plane in range(2):
        slot = jnp.where(me == 0, plane, 0)
        for j2a in range(4):
            parts = []
            for m2lo in range(2):
                for p_high in range(4):
                    first = p_high * 32 + (j2a // 2) * 16
                    parts.append(s_recv[slot, pl.ds(first, 16), (j2a % 2) * 2 + m2lo, :])
            scale[plane, j2a] = jnp.concatenate(parts, 0).T

    for load in loads[3:]:
        load.wait()

    @pl.loop(0, 2)
    def _(f):
        finish(f_recv.at[f, pl.ds(0, 127 * 8)], recv_sems.at[2 + f])
        for part in range(2):
            values = jnp.concatenate([
                jnp.concatenate([
                    f_recv[f, pl.ds(ri * 4 + part * 2 + l, 128, stride=8), :] for l in range(2)], 1)
                for ri in range(2)], 0)
            high, low = split(values)
            y_mid[:, part * 256:(part + 1) * 256] = (
                dot(tables[T_P, 0], high) + dot(tables[T_P, 0], low) + dot(tables[T_P, 1], high))

        @pl.loop(0, 8)
        def _(n):
            at = pl.multiple_of(n * 16, 16)
            real, imag = [], []
            for l in range(4):
                lanes = slice(l * 128, (l + 1) * 128)
                vr, vi = y_mid[pl.ds(at, 16), lanes], y_mid[pl.ds(128 + at, 16), lanes]
                wr, wi = twiddle[0, pl.ds(at, 16), lanes], twiddle[1, pl.ds(at, 16), lanes]
                real.append(vr * wr - vi * wi)
                imag.append(vr * wi + vi * wr)
            r02, r13 = real[0] + real[2], real[1] + real[3]
            i02, i13 = imag[0] + imag[2], imag[1] + imag[3]
            rd, re = real[0] - real[2], real[1] - real[3]
            id_, ie = imag[0] - imag[2], imag[1] - imag[3]
            outs = ((r02 + r13, i02 + i13), (rd + ie, id_ - re), (r02 - r13, i02 - i13), (rd - ie, id_ + re))
            for j2a, pair in enumerate(outs):
                for ri in range(2):
                    high, low = split(pair[ri])
                    v_high[j2a, pl.ds(at, 16), ri * 128:(ri + 1) * 128] = high
                    v_low[j2a, pl.ds(at, 16), ri * 128:(ri + 1) * 128] = low

        for j2a in range(4):
            high, low = v_high[j2a], v_low[j2a]
            spectral = (dot(high, tables[T_C + j2a, 0]) + dot(low, tables[T_C + j2a, 0])
                        + dot(high, tables[T_C + j2a, 1]))
            factor = scale[f, j2a]
            high, low = split(spectral * jnp.concatenate([factor, factor], 1))
            v_back[j2a] = (dot(high, tables[T_CI + j2a, 0]) + dot(low, tables[T_CI + j2a, 0])
                           + dot(high, tables[T_CI + j2a, 1]))

        @pl.loop(0, 8)
        def _(n):
            at = pl.multiple_of(n * 16, 16)
            real = [v_back[j2a, pl.ds(at, 16), 0:128] for j2a in range(4)]
            imag = [v_back[j2a, pl.ds(at, 16), 128:256] for j2a in range(4)]
            r02, r13 = real[0] + real[2], real[1] + real[3]
            i02, i13 = imag[0] + imag[2], imag[1] + imag[3]
            rd, re = real[0] - real[2], real[1] - real[3]
            id_, ie = imag[0] - imag[2], imag[1] - imag[3]
            outs = ((r02 + r13, i02 + i13), (rd - ie, id_ + re), (r02 - r13, i02 - i13), (rd + ie, id_ - re))
            for l, (vr, vi) in enumerate(outs):
                lanes = slice(l * 128, (l + 1) * 128)
                wr, wi = twiddle[0, pl.ds(at, 16), lanes], twiddle[1, pl.ds(at, 16), lanes]
                for ri, value in enumerate((vr * wr + vi * wi, vi * wr - vr * wi)):
                    high, low = split(value)
                    z_high[pl.ds(ri * 128 + at, 16), lanes] = high
                    z_low[pl.ds(ri * 128 + at, 16), lanes] = low

        for part in range(2):
            high, low = z_high[:, part * 256:(part + 1) * 256], z_low[:, part * 256:(part + 1) * 256]
            out = dot(tables[T_PI, 0], high) + dot(tables[T_PI, 0], low) + dot(tables[T_PI, 1], high)
            for ri in range(2):
                for l in range(2):
                    b_send[f, pl.ds(ri * 4 + part * 2 + l, 128, stride=8), :] = (
                        out[ri * 128:(ri + 1) * 128, l * 128:(l + 1) * 128])
        send_all(lambda d: b_send.at[f, block_of(d)], lambda m: b_recv.at[f, block_of(m)], 4 + f)
        b_recv[f, block_of(me), :] = b_send[f, block_of(me), :]

    for f in range(2):
        finish(b_recv.at[f, pl.ds(0, 127 * 8)], recv_sems.at[4 + f])
    swap_first(b_recv)

    def over_column(action):
        for dx in (2, 1, 3, 0):
            for dz in (1, 0):
                for dc in (1, 0):
                    if (dx, dz, dc) != (0, 0, 0):
                        action(lax.rem(x + dx, 4) * 4 + lax.rem(zl + dz, 2) * 2 + lax.rem(c + dc, 2))

    @pl.loop(0, 2)
    def _(f):
        for l in range(4):
            cells = pl.ds(l * 128, 128)
            values = jnp.concatenate(
                [b_recv[f, pl.ds(ri * 4 + l, 128, stride=8), :].T for ri in range(2)], 1)
            high, low = split(values)
            fields = dot(high, tables[T_U, 0]) + dot(low, tables[T_U, 0]) + dot(high, tables[T_U, 1])
            modulus = jnp.exp(0.5 * fields)
            modulus_ref[f, cells, :] = modulus
            high, low = split(modulus)
            high, low = split(dot(high, pairs[...]) + dot(low, pairs[...]))
            g_high[cells, :] = high
            g_low[cells, :] = low
        coarse = dot(rows[...], g_high[...]) + dot(rows[...], g_low[...])
        for i in range(8):
            r_send[f * 8 + i, pl.ds(0, 16), :] = coarse[i * PIECE:i * PIECE + 16, 0:128]
            r_send[f * 8 + i, pl.ds(16, 8), :] = coarse[i * PIECE + 16:(i + 1) * PIECE, 128:256]

    over_column(lambda g: pltpu.make_async_remote_copy(
        r_send.at[g], r_recv.at[column], send_sems.at[6], recv_sems.at[6],
        device_id=line + g, device_id_type=LOGICAL).start())
    r_recv[column] = r_send[column]
    finish(r_recv.at[pl.ds(0, 15)], recv_sems.at[6])

    lower = lax.broadcasted_iota(jnp.int32, (8, 128), 0) < 4

    @pl.loop(0, 16)
    def _(g):
        t_send[g, pl.ds(0, 16), :] = r_recv[order_ref[0, g], pl.ds(0, 16), :]
        second = r_recv[order_ref[1, g], pl.ds(16, 8), :]
        third = r_recv[order_ref[2, g], pl.ds(16, 8), :]
        t_send[g, pl.ds(16, 8), :] = jnp.where(lower, second, third)

    over_column(lambda g: pltpu.make_async_remote_copy(
        t_send.at[g], t_recv.at[column], send_sems.at[7], recv_sems.at[7],
        device_id=line + g, device_id_type=LOGICAL).start())
    t_recv[column] = t_send[column]
    finish(t_recv.at[pl.ds(0, 15)], recv_sems.at[7])
    for i in range(16):
        one_ref[pl.ds(i * 16, 16), :] = t_recv[i, pl.ds(0, 16), :]
        tail = t_recv[i, pl.ds(16, 8), :]
        two_ref[pl.ds(i * 4, 4), :] = tail[0:4, 0:64]
        three_ref[pl.ds(i, 1), :] = tail[4:5, 64:96]

    finish(s_send.at[pl.ds(0, 127)], send_sems.at[0])

    @pl.when(me != 0)
    def _():
        finish(n_send.at[0], send_sems.at[1])

    for f in range(2):
        finish(f_send.at[f, pl.ds(0, 127 * 8)], send_sems.at[2 + f])
        finish(b_send.at[f, pl.ds(0, 127 * 8)], send_sems.at[4 + f])
    finish(r_send.at[pl.ds(0, 15)], send_sems.at[6])
    finish(t_send.at[pl.ds(0, 15)], send_sems.at[7])


def on_device(white_noise, spectrum, group_table):
    tables, twiddle, pairs, rows = build_tables()
    anywhere = pl.BlockSpec(memory_space=pl.ANY)
    vmem = pl.BlockSpec(memory_space=pltpu.VMEM)
    modulus, one, two, three = pl.pallas_call(
        kernel,
        out_shape=(
            jax.ShapeDtypeStruct((2, CELLS, NZ), F32),
            jax.ShapeDtypeStruct((256, 128), F32),
            jax.ShapeDtypeStruct((64, 64), F32),
            jax.ShapeDtypeStruct((16, 32), F32),
        ),
        in_specs=[anywhere, anywhere, pl.BlockSpec(memory_space=pltpu.SMEM)] + [anywhere] * 4,
        out_specs=(vmem, vmem, vmem, vmem),
        scratch_shapes=[
            pltpu.VMEM((2, CELLS, NZ), F32),
            pltpu.VMEM((CELLS, NZ), F32),
            pltpu.VMEM((TABLES, 2, 256, 256), BF16),
            pltpu.VMEM((2, 128, CELLS), F32),
            pltpu.VMEM((NZ, 256), BF16),
            pltpu.VMEM((8 * PIECE, CELLS), BF16),
            pltpu.VMEM((128, 4, 128), F32),
            pltpu.VMEM((2, 128, 4, 128), F32),
            pltpu.VMEM((1, 4, 128), F32),
            pltpu.VMEM((2, 4, 128, 128), F32),
            pltpu.VMEM((2, 1024, 128), F32),
            pltpu.VMEM((2, 1024, 128), F32),
            pltpu.VMEM((2, 1024, 128), F32),
            pltpu.VMEM((2, 1024, 128), F32),
            pltpu.VMEM((256, CELLS), F32),
            pltpu.VMEM((4, 128, 256), BF16),
            pltpu.VMEM((4, 128, 256), BF16),
            pltpu.VMEM((4, 128, 256), F32),
            pltpu.VMEM((256, CELLS), BF16),
            pltpu.VMEM((256, CELLS), BF16),
            pltpu.VMEM((CELLS, 256), BF16),
            pltpu.VMEM((CELLS, 256), BF16),
            pltpu.VMEM((16, PIECE, 128), F32),
            pltpu.VMEM((16, PIECE, 128), F32),
            pltpu.VMEM((16, PIECE, 128), F32),
            pltpu.VMEM((16, PIECE, 128), F32),
            pltpu.SemaphoreType.DMA((7,)),
            pltpu.SemaphoreType.DMA((8,)),
            pltpu.SemaphoreType.DMA((8,)),
        ],
        compiler_params=pltpu.CompilerParams(
            collective_id=0, has_side_effects=True, vmem_limit_bytes=48 << 20),
        name="moduli",
    )(
        white_noise.reshape(2, CELLS, NZ), spectrum.reshape(CELLS, NZ), group_table,
        jnp.asarray(tables), jnp.asarray(twiddle), jnp.asarray(pairs), jnp.asarray(rows),
    )
    return (
        modulus.reshape(2, CX, CY, NZ),
        one.reshape(2, 8, 16, 128),
        two.reshape(2, 4, 8, 64),
        three.reshape(2, 2, 4, 32),
    )


def solution(mesh):
    split_mesh = Mesh(mesh.devices.reshape(2, 4, 4, 2, 2), (*PX, *PY))
    whole = P(None, PX, PY, None)
    return jax.shard_map(
        on_device,
        mesh=split_mesh,
        in_specs=(whole, P(PX, PY, None), P()),
        out_specs=(whole, whole, whole, whole),
        check_vma=False,
    )
```

```python
import functools

import jax
import jax.numpy as jnp
import ml_dtypes
import numpy as np
from jax import lax
from jax.experimental import pallas as pl
from jax.experimental.pallas import tpu as pltpu
from jax.sharding import Mesh
from jax.sharding import PartitionSpec as P

PX = ("px_0", "px_1")
PY = ("py_0", "py_1", "py_2")
F32 = jnp.float32
BF16 = jnp.bfloat16
LOGICAL = pl.DeviceIdType.LOGICAL

NX, NY, NZ = 128, 512, 256
CX, CY = 16, 32
CELLS = CX * CY
T_Z, T_P, T_C, T_CI, T_PI, T_U, TABLES = 0, 1, 2, 6, 10, 11, 12


def wave(products, length, sign):
    angles = 2.0 * np.pi * (products % length) / length
    return np.cos(angles), sign * np.sin(angles)


def applied_left(real, imag):
    return np.block([[real, -imag], [imag, real]])


def build_tables():
    spots = np.arange(128)
    z = np.arange(NZ)
    p, q = spots // 16, spots % 16
    j1, m1 = spots // 16, spots % 16
    tables = np.zeros((TABLES, 256, 256))
    cos_z, sin_z = wave(spots[:, None] * z[None, :], NZ, -1.0)
    sin_z[0] = (-1.0) ** z
    tables[T_Z] = np.concatenate([cos_z, sin_z], 0)
    weight = np.where(spots == 0, 1.0, 2.0)[:, None] / float(NX * NY * NZ)
    tables[T_U] = np.concatenate([cos_z * weight, sin_z * weight], 0)
    outer = 2 * p[None, :] * j1[:, None] + q[None, :] * m1[:, None]
    tables[T_P] = applied_left(*wave(outer, 16, -1.0))
    tables[T_PI] = applied_left(*wave(outer.T, 16, 1.0))
    low, b = spots // 32, spots % 32
    half, j2b, q2 = spots // 64, (spots // 16) % 4, spots % 16
    m2 = 2 * q2 + half
    for j2a in range(4):
        inner = 2 * low[:, None] * j2a + 8 * low[:, None] * j2b[None, :] + b[:, None] * m2[None, :]
        tables[T_C + j2a] = applied_left(*wave(inner.T, 32, -1.0)).T
        tables[T_CI + j2a] = applied_left(*wave(inner, 32, 1.0)).T
    cell_a, cell_b = np.arange(CELLS) // CY, np.arange(CELLS) % CY
    middle = 4 * cell_a[None, :] * j1[:, None] + cell_b[None, :] * m1[:, None]
    twiddle = np.stack(wave(middle, 512, -1.0)).astype(np.float32)
    high = tables.astype(np.float32).astype(ml_dtypes.bfloat16)
    rest = (tables - high.astype(np.float64)).astype(np.float32).astype(ml_dtypes.bfloat16)
    pairs = np.zeros((NZ, 256))
    pairs[z, z // 2] = 0.5
    pairs[z, 128 + z // 4] = 0.25
    pairs[z, 192 + z // 8] = 0.125
    rows = np.zeros((192, CELLS))
    for cell in range(CELLS):
        a, b = divmod(cell, CY)
        rows[(a // 2) * 16 + b // 2, cell] = 0.25
        rows[128 + (a // 4) * 8 + b // 4, cell] = 1.0 / 16
        rows[160 + 2 * ((a // 8) * 4 + b // 8), cell] = 1.0 / 64
    exact = ml_dtypes.bfloat16
    return np.stack([high, rest], 1), twiddle, pairs.astype(exact), rows.astype(exact)


def dot(left, right):
    return jnp.dot(left, right, preferred_element_type=F32)


def dot_nt(left, right):
    return lax.dot_general(left, right, (((1,), (1,)), ((), ())), preferred_element_type=F32)


def split(values):
    high = values.astype(BF16)
    return high, (values - high.astype(F32)).astype(BF16)


def ordered(index):
    return lax.rem(2 - index + 3 * (index // 2) + 2 * (index // 3) + 4, 4)


def kernel(
    noise_hbm, spec_hbm, order_hbm, tables_hbm, twiddle_hbm, pairs_hbm, rows_hbm,
    modulus_ref, fine_ref, rest_ref,
    order_smem, noise, spec, tables, twiddle, pairs, rows,
    s_send, s_recv, n_send, scale, f_send, f_recv, b_send, b_recv,
    y_mid, v_high, v_low, v_back, z_high, z_low, g_high, g_low,
    r_send, r_recv, r_other, r_send_rest, r_recv_rest, r_other_rest, t_send, t_recv, t_send_rest, t_recv_rest,
    load_sems, send_sems, recv_sems, route_send_sems, route_recv_sems,
):
    zh, y, x, zl, c = [lax.axis_index(a) for a in (*PX, *PY)]
    z = zh * 2 + zl
    line = zh * 64 + y * 16
    column = x * 4 + zl * 2 + c
    me = line + column

    loads = []
    for k, (source, target) in enumerate((
        (spec_hbm, spec), (tables_hbm.at[T_Z], tables.at[T_Z]), (noise_hbm, noise),
        (tables_hbm.at[pl.ds(1, TABLES - 1)], tables.at[pl.ds(1, TABLES - 1)]),
        (twiddle_hbm, twiddle), (pairs_hbm, pairs), (rows_hbm, rows), (order_hbm, order_smem),
    )):
        load = pltpu.make_async_copy(source, target, load_sems.at[k])
        load.start()
        loads.append(load)

    def over_half(action, half):
        core = lax.rem(c + 1 - half, 2)

        def group(s, skip):
            z2 = lax.rem(z + ordered(s), 4)
            base = (z2 // 2) * 64 + lax.rem(z2, 2) * 2 + core
            ys = [lax.rem(y + ordered(lax.rem(s + t, 4)), 4) * 16 for t in range(4)]
            xs = [lax.rem(x + ordered(lax.rem(s + t, 4)), 4) * 4 for t in range(4)]
            for t in range(4):
                for u in range(4):
                    if not (skip and t == 0 and u == 0):
                        action(base + ys[t] + xs[u])

        @pl.loop(0, 4 - half)
        def _(s):
            group(s, False)

        if half:
            group(jnp.int32(3), True)

    def over_devices(action):
        over_half(action, 0)
        over_half(action, 1)

    barrier = pltpu.get_barrier_semaphore()
    over_devices(lambda d: pl.semaphore_signal(barrier, 1, device_id=d, device_id_type=LOGICAL))

    def send(source, target, send_sem, recv_sem):
        return lambda d: pltpu.make_async_remote_copy(
            source(d), target, send_sem, recv_sem, device_id=d, device_id_type=LOGICAL).start()

    def finish(ref, sem):
        pltpu.make_async_copy(ref, ref, sem).wait()

    loads[0].wait()
    for jj in range(4):
        j2lo, m2lo = divmod(jj, 2)
        starts = [(j2lo * 8 + j1) * CY + m2lo * 16 for j1 in range(8)]
        block = jnp.concatenate([spec[pl.ds(s, 16), 0:128] for s in starts], 0)
        s_send[:, jj, :] = block.T
        block = jnp.concatenate([spec[pl.ds(s, 16), 128:256] for s in starts], 0)
        n_send[0, jj, :] = block.T[0]

    loads[1].wait()
    loads[2].wait()

    @pl.loop(0, 2)
    def _(f):
        for part in range(2):
            high, low = split(noise[f, pl.ds(part * 256, 256), :])
            out = dot_nt(tables[T_Z, 0], high) + dot_nt(tables[T_Z, 0], low) + dot_nt(tables[T_Z, 1], high)
            for ri in range(2):
                for l in range(2):
                    f_send[f, pl.ds(ri * 4 + part * 2 + l, 128, stride=8), :] = (
                        out[ri * 128:(ri + 1) * 128, l * 128:(l + 1) * 128])

    def swap_first(ref):
        first, second = ref[0, pl.ds(0, 8), :], ref[1, pl.ds(0, 8), :]
        ref[0, pl.ds(0, 8), :] = jnp.concatenate([first[:4], second[:4]], 0)
        ref[1, pl.ds(0, 8), :] = jnp.concatenate([first[4:], second[4:]], 0)

    def block_of(d):
        return pl.ds(pl.multiple_of(d * 8, 8), 8)

    swap_first(f_send)
    pl.semaphore_wait(barrier, 127)
    over_devices(send(lambda d: s_send.at[d], s_recv.at[0, me], send_sems.at[0], recv_sems.at[0]))
    s_recv[0, me] = s_send[me]

    @pl.when(me == 0)
    def _():
        s_recv[1, 0] = n_send[0]

    def send_forward(f, half):
        over_half(send(
            lambda d: f_send.at[f, block_of(d)], f_recv.at[f, block_of(me)],
            send_sems.at[2 + 2 * f + half], recv_sems.at[2 + f]), half)

    def forward_sent(f, half):
        finish(f_send.at[f, pl.ds(0, (64 - half) * 8)], send_sems.at[2 + 2 * f + half])

    send_forward(0, 0)
    send_forward(0, 1)
    send_forward(1, 0)
    send_forward(1, 1)
    @pl.when(me != 0)
    def _():
        pltpu.make_async_remote_copy(
            n_send.at[0], s_recv.at[1, me], send_sems.at[1], recv_sems.at[1],
            device_id=jnp.int32(0), device_id_type=LOGICAL).start()

    for f in range(2):
        f_recv[f, block_of(me), :] = f_send[f, block_of(me), :]

    finish(s_recv.at[0, pl.ds(0, 127)], recv_sems.at[0])

    def arrange(plane):
        for j2a in range(4):
            parts = []
            for m2lo in range(2):
                for p_high in range(4):
                    first = p_high * 32 + (j2a // 2) * 16
                    parts.append(s_recv[plane, pl.ds(first, 16), (j2a % 2) * 2 + m2lo, :])
            scale[plane, j2a] = jnp.concatenate(parts, 0).T

    arrange(0)
    for load in loads[3:]:
        load.wait()

    def send_back(f):
        over_devices(send(
            lambda d: b_send.at[f, block_of(d)], b_recv.at[f, block_of(me)],
            send_sems.at[6 + f], recv_sems.at[4 + f]))

    @pl.loop(0, 2)
    def _(f):
        finish(f_recv.at[f, pl.ds(0, 127 * 8)], recv_sems.at[2 + f])
        @pl.when(jnp.logical_and(me == 0, f == 1))
        def _():
            finish(s_recv.at[1, pl.ds(0, 127)], recv_sems.at[1])
            arrange(1)

        for part in range(2):
            values = jnp.concatenate([
                jnp.concatenate([
                    f_recv[f, pl.ds(ri * 4 + part * 2 + l, 128, stride=8), :] for l in range(2)], 1)
                for ri in range(2)], 0)
            high, low = split(values)
            y_mid[:, part * 256:(part + 1) * 256] = (
                dot(tables[T_P, 0], high) + dot(tables[T_P, 0], low) + dot(tables[T_P, 1], high))

        @pl.loop(0, 8)
        def _(n):
            at = pl.multiple_of(n * 16, 16)
            real, imag = [], []
            for l in range(4):
                lanes = slice(l * 128, (l + 1) * 128)
                vr, vi = y_mid[pl.ds(at, 16), lanes], y_mid[pl.ds(128 + at, 16), lanes]
                wr, wi = twiddle[0, pl.ds(at, 16), lanes], twiddle[1, pl.ds(at, 16), lanes]
                real.append(vr * wr - vi * wi)
                imag.append(vr * wi + vi * wr)
            r02, r13 = real[0] + real[2], real[1] + real[3]
            i02, i13 = imag[0] + imag[2], imag[1] + imag[3]
            rd, re = real[0] - real[2], real[1] - real[3]
            id_, ie = imag[0] - imag[2], imag[1] - imag[3]
            outs = ((r02 + r13, i02 + i13), (rd + ie, id_ - re), (r02 - r13, i02 - i13), (rd - ie, id_ + re))
            for j2a, pair in enumerate(outs):
                for ri in range(2):
                    high, low = split(pair[ri])
                    v_high[j2a, pl.ds(at, 16), ri * 128:(ri + 1) * 128] = high
                    v_low[j2a, pl.ds(at, 16), ri * 128:(ri + 1) * 128] = low

        for j2a in range(4):
            high, low = v_high[j2a], v_low[j2a]
            spectral = (dot(high, tables[T_C + j2a, 0]) + dot(low, tables[T_C + j2a, 0])
                        + dot(high, tables[T_C + j2a, 1]))
            factor = scale[jnp.where(me == 0, f, 0), j2a]
            high, low = split(spectral * jnp.concatenate([factor, factor], 1))
            v_back[j2a] = (dot(high, tables[T_CI + j2a, 0]) + dot(low, tables[T_CI + j2a, 0])
                           + dot(high, tables[T_CI + j2a, 1]))

        @pl.loop(0, 8)
        def _(n):
            at = pl.multiple_of(n * 16, 16)
            real = [v_back[j2a, pl.ds(at, 16), 0:128] for j2a in range(4)]
            imag = [v_back[j2a, pl.ds(at, 16), 128:256] for j2a in range(4)]
            r02, r13 = real[0] + real[2], real[1] + real[3]
            i02, i13 = imag[0] + imag[2], imag[1] + imag[3]
            rd, re = real[0] - real[2], real[1] - real[3]
            id_, ie = imag[0] - imag[2], imag[1] - imag[3]
            outs = ((r02 + r13, i02 + i13), (rd - ie, id_ + re), (r02 - r13, i02 - i13), (rd + ie, id_ - re))
            for l, (vr, vi) in enumerate(outs):
                lanes = slice(l * 128, (l + 1) * 128)
                wr, wi = twiddle[0, pl.ds(at, 16), lanes], twiddle[1, pl.ds(at, 16), lanes]
                for ri, value in enumerate((vr * wr + vi * wi, vi * wr - vr * wi)):
                    high, low = split(value)
                    z_high[pl.ds(ri * 128 + at, 16), lanes] = high
                    z_low[pl.ds(ri * 128 + at, 16), lanes] = low

        for part in range(2):
            high, low = z_high[:, part * 256:(part + 1) * 256], z_low[:, part * 256:(part + 1) * 256]
            out = dot(tables[T_PI, 0], high) + dot(tables[T_PI, 0], low) + dot(tables[T_PI, 1], high)
            for ri in range(2):
                for l in range(2):
                    half, row = jnp.where(me == 0, ri, f), jnp.where(me == 0, f, ri)
                    b_send[half, pl.ds(row * 4 + part * 2 + l, 128, stride=8), :] = (
                        out[ri * 128:(ri + 1) * 128, l * 128:(l + 1) * 128])

        @pl.when(jnp.logical_or(me != 0, f == 1))
        def _():
            send_back(f)

    @pl.when(me == 0)
    def _():
        send_back(0)

    for f in range(2):
        b_recv[f, block_of(me), :] = b_send[f, block_of(me), :]

    def over_column(action):
        for dx in (2, 1, 3, 0):
            for dz in (1, 0):
                for dc in (1, 0):
                    if (dx, dz, dc) != (0, 0, 0):
                        action(lax.rem(x + dx, 4) * 4 + lax.rem(zl + dz, 2) * 2 + lax.rem(c + dc, 2))

    def send_pieces(f, phase, pairs_of_refs):
        over_column(lambda g: [pltpu.make_async_remote_copy(
            source.at[g], target.at[column], route_send_sems.at[phase + k, f], route_recv_sems.at[phase + k, f],
            device_id=line + g, device_id_type=LOGICAL).start()
            for k, (source, target) in enumerate(pairs_of_refs)])
        for source, target in pairs_of_refs:
            target[column] = source[column]

    def await_pieces(f, phase, pairs_of_refs):
        for k, (_, target) in enumerate(pairs_of_refs):
            finish(target.at[pl.ds(0, 15)], route_recv_sems.at[phase + k, f])

    first_refs = [((r_send.at[0], r_recv), (r_send_rest.at[0], r_recv_rest)),
                  ((r_send.at[1], r_other), (r_send_rest.at[1], r_other_rest))]
    second_refs = [((t_send.at[f], t_recv.at[f]), (t_send_rest.at[f], t_recv_rest.at[f])) for f in range(2)]

    fewer = lax.broadcasted_iota(jnp.int32, (32, 128), 1) < 64

    for f in range(2):
        finish(b_recv.at[f, pl.ds(0, 127 * 8)], recv_sems.at[4 + f])
        for l in range(4):
            cells = pl.ds(l * 128, 128)
            values = jnp.concatenate(
                [b_recv[f, pl.ds(ri * 4 + l, 128, stride=8), :].T for ri in range(2)], 1)
            high, low = split(values)
            fields = dot(high, tables[T_U, 0]) + dot(low, tables[T_U, 0]) + dot(high, tables[T_U, 1])
            modulus = jnp.exp(0.5 * fields)
            modulus_ref[f, cells, :] = modulus
            high, low = split(modulus)
            high, low = split(dot(high, pairs[...]) + dot(low, pairs[...]))
            g_high[cells, :] = high
            g_low[cells, :] = low
        coarse = dot(rows[...], g_high[...]) + dot(rows[...], g_low[...])
        r_send[f] = coarse[0:128, 0:128].reshape(16, 8, 128)
        r_send_rest[f] = jnp.where(fewer, coarse[128:160, 128:256], coarse[160:192, 128:256]).reshape(16, 2, 128)
        send_pieces(f, 0, first_refs[f])

    for f in range(2):
        await_pieces(f, 0, first_refs[f])
        (_, held), (_, held_rest) = first_refs[f]

        @pl.loop(0, 16)
        def _(g):
            t_send[f, g] = held[order_smem[0, g]]
            second, third = held_rest[order_smem[1, g]], held_rest[order_smem[2, g]]
            t_send_rest[f, g] = jnp.where(fewer[0:2], second, third)

        send_pieces(f, 2, second_refs[f])

    for f in range(2):
        await_pieces(f, 2, second_refs[f])
        fine_ref[f] = t_recv[f]
        rest_ref[f] = t_recv_rest[f]

    finish(s_send.at[pl.ds(0, 127)], send_sems.at[0])

    @pl.when(me != 0)
    def _():
        finish(n_send.at[0], send_sems.at[1])

    for f in range(2):
        finish(b_send.at[f, pl.ds(0, 127 * 8)], send_sems.at[6 + f])
        for k, (whole, rest) in enumerate(((r_send, r_send_rest), (t_send, t_send_rest))):
            finish(whole.at[f, pl.ds(0, 15)], route_send_sems.at[2 * k, f])
            finish(rest.at[f, pl.ds(0, 15)], route_send_sems.at[2 * k + 1, f])
    for f in range(2):
        for half in range(2):
            forward_sent(f, half)


def finisher(modulus_ref, fine_ref, rest_ref, modulus_hbm, one_ref, two_ref, three_ref, sem):
    store = pltpu.make_async_copy(modulus_ref, modulus_hbm, sem)
    store.start()
    for f in range(2):
        one_ref[pl.ds(f * 128, 128), :] = fine_ref[f].reshape(128, 128)
        rest = rest_ref[f]
        two_ref[pl.ds(f * 32, 32), :] = rest.reshape(32, 128)[:, 0:64]
        three_ref[pl.ds(f * 8, 8), :] = rest[0:8, 0, 64:96]
    store.wait()


def on_device(white_noise, spectrum, group_table):
    tables, twiddle, pairs, rows = build_tables()
    hbm = pl.BlockSpec(memory_space=pltpu.HBM)
    vmem = pl.BlockSpec(memory_space=pltpu.VMEM)
    modulus_shape = jax.ShapeDtypeStruct((2, CELLS, NZ), F32)
    modulus, fine, rest = pl.pallas_call(
        kernel,
        out_shape=(pltpu.VMEM((2, CELLS, NZ), F32), pltpu.VMEM((2, 16, 8, 128), F32), pltpu.VMEM((2, 16, 2, 128), F32)),
        in_specs=[hbm] * 7,
        out_specs=(vmem, vmem, vmem),
        scratch_shapes=[
            pltpu.SMEM((3, 16), jnp.int32),
            pltpu.VMEM((2, CELLS, NZ), F32),
            pltpu.VMEM((CELLS, NZ), F32),
            pltpu.VMEM((TABLES, 2, 256, 256), BF16),
            pltpu.VMEM((2, 128, CELLS), F32),
            pltpu.VMEM((NZ, 256), BF16),
            pltpu.VMEM((192, CELLS), BF16),
            pltpu.VMEM((128, 4, 128), F32),
            pltpu.VMEM((2, 128, 4, 128), F32),
            pltpu.VMEM((1, 4, 128), F32),
            pltpu.VMEM((2, 4, 128, 128), F32),
            pltpu.VMEM((2, 1024, 128), F32),
            pltpu.VMEM((2, 1024, 128), F32),
            pltpu.VMEM((2, 1024, 128), F32),
            pltpu.VMEM((2, 1024, 128), F32),
            pltpu.VMEM((256, CELLS), F32),
            pltpu.VMEM((4, 128, 256), BF16),
            pltpu.VMEM((4, 128, 256), BF16),
            pltpu.VMEM((4, 128, 256), F32),
            pltpu.VMEM((256, CELLS), BF16),
            pltpu.VMEM((256, CELLS), BF16),
            pltpu.VMEM((CELLS, 256), BF16),
            pltpu.VMEM((CELLS, 256), BF16),
            *[pltpu.VMEM((*count, 16, size, 128), F32) for size in (8, 2) for count in ((2,), (), ())],
            *[pltpu.VMEM((2, 16, size, 128), F32) for size in (8, 8, 2, 2)],
            pltpu.SemaphoreType.DMA((8,)),
            pltpu.SemaphoreType.DMA((8,)),
            pltpu.SemaphoreType.DMA((6,)),
            pltpu.SemaphoreType.DMA((4, 2)),
            pltpu.SemaphoreType.DMA((4, 2)),
        ],
        compiler_params=pltpu.CompilerParams(
            collective_id=0, has_side_effects=True, vmem_limit_bytes=60000000),
        name="moduli",
    )(
        white_noise.reshape(2, CELLS, NZ), spectrum.reshape(CELLS, NZ), group_table,
        jnp.asarray(tables), jnp.asarray(twiddle), jnp.asarray(pairs), jnp.asarray(rows),
    )
    modulus, one, two, three = pl.pallas_call(
        finisher,
        out_shape=(
            modulus_shape,
            jax.ShapeDtypeStruct((256, 128), F32),
            jax.ShapeDtypeStruct((64, 64), F32),
            jax.ShapeDtypeStruct((16, 32), F32),
        ),
        in_specs=[vmem, vmem, vmem],
        out_specs=(hbm, vmem, vmem, vmem),
        scratch_shapes=[pltpu.SemaphoreType.DMA],
        compiler_params=pltpu.CompilerParams(vmem_limit_bytes=4 << 20),
        name="levels",
    )(modulus, fine, rest)
    return (
        modulus.reshape(2, CX, CY, NZ),
        one.reshape(2, 8, 16, 128),
        two.reshape(2, 4, 8, 64),
        three.reshape(2, 2, 4, 32),
    )


def solution(mesh):
    split_mesh = Mesh(mesh.devices.reshape(2, 4, 4, 2, 2), (*PX, *PY))
    whole = P(None, PX, PY, None)
    return jax.shard_map(
        on_device,
        mesh=split_mesh,
        in_specs=(whole, P(PX, PY, None), P()),
        out_specs=(whole, whole, whole, whole),
        check_vma=False,
    )
```

```python
import functools

import jax
import jax.numpy as jnp
import ml_dtypes
import numpy as np
from jax import lax
from jax.experimental import pallas as pl
from jax.experimental.pallas import tpu as pltpu
from jax.sharding import Mesh
from jax.sharding import PartitionSpec as P

PX = ("px_0", "px_1")
PY = ("py_0", "py_1", "py_2")
F32 = jnp.float32
BF16 = jnp.bfloat16
LOGICAL = pl.DeviceIdType.LOGICAL

NX, NY, NZ = 128, 512, 256
CX, CY = 16, 32
CELLS = CX * CY
T_Z, T_P, T_C, T_PI, T_U, TABLES = 0, 1, 2, 6, 7, 8


def wave(products, length, sign):
    angles = 2.0 * np.pi * (products % length) / length
    return np.cos(angles), sign * np.sin(angles)


def applied_left(real, imag):
    return np.block([[real, -imag], [imag, real]])


def build_tables():
    spots = np.arange(128)
    z = np.arange(NZ)
    p, q = spots // 16, spots % 16
    j1, m1 = spots // 16, spots % 16
    tables = np.zeros((TABLES, 256, 256))
    cos_z, sin_z = wave(spots[:, None] * z[None, :], NZ, -1.0)
    sin_z[0] = (-1.0) ** z
    tables[T_Z] = np.concatenate([cos_z, sin_z], 0)
    weight = np.where(spots == 0, 1.0, 2.0)[:, None] / float(NX * NY * NZ)
    tables[T_U] = np.concatenate([cos_z * weight, sin_z * weight], 0)
    outer = 2 * p[None, :] * j1[:, None] + q[None, :] * m1[:, None]
    tables[T_P] = applied_left(*wave(outer, 16, -1.0))
    tables[T_PI] = applied_left(*wave(outer.T, 16, 1.0))
    low, b = spots // 32, spots % 32
    half, j2b, q2 = spots // 64, (spots // 16) % 4, spots % 16
    m2 = 2 * q2 + half
    for j2a in range(4):
        inner = 2 * low[:, None] * j2a + 8 * low[:, None] * j2b[None, :] + b[:, None] * m2[None, :]
        tables[T_C + j2a] = applied_left(*wave(inner.T, 32, -1.0)).T
    cell_a, cell_b = np.arange(CELLS) // CY, np.arange(CELLS) % CY
    middle = 4 * cell_a[None, :] * j1[:, None] + cell_b[None, :] * m1[:, None]
    twiddle = np.stack(wave(middle, 512, -1.0)).astype(np.float32)
    high = tables.astype(np.float32).astype(ml_dtypes.bfloat16)
    rest = (tables - high.astype(np.float64)).astype(np.float32).astype(ml_dtypes.bfloat16)
    pairs = np.zeros((NZ, 256))
    pairs[z, z // 2] = 0.5
    pairs[z, 128 + z // 4] = 0.25
    pairs[z, 192 + z // 8] = 0.125
    rows = np.zeros((192, CELLS))
    for cell in range(CELLS):
        a, b = divmod(cell, CY)
        rows[(a // 2) * 16 + b // 2, cell] = 0.25
        rows[128 + (a // 4) * 8 + b // 4, cell] = 1.0 / 16
        rows[160 + 2 * ((a // 8) * 4 + b // 8), cell] = 1.0 / 64
    exact = ml_dtypes.bfloat16
    return np.stack([high, rest], 1), twiddle, pairs.astype(exact), rows.astype(exact)


def dot(left, right):
    return jnp.dot(left, right, preferred_element_type=F32)


def dot_nt(left, right):
    return lax.dot_general(left, right, (((1,), (1,)), ((), ())), preferred_element_type=F32)


def split(values):
    high = values.astype(BF16)
    return high, (values - high.astype(F32)).astype(BF16)


def ordered(index):
    return lax.rem(2 - index + 3 * (index // 2) + 2 * (index // 3) + 4, 4)


def kernel(
    noise_hbm, spec_hbm, order_hbm, tables_hbm, twiddle_hbm, pairs_hbm, rows_hbm,
    modulus_ref, fine_ref, rest_ref,
    order_smem, noise, spec, tables, twiddle, pairs, rows,
    tables_back, s_send, s_recv, n_send, n_recv, mirrored, reversed_, wrapped, scale, f_send, f_recv, b_send, b_recv,
    y_mid, v_high, v_low, v_back, z_high, z_low, g_high, g_low,
    r_send, r_recv, r_other, r_send_rest, r_recv_rest, r_other_rest, t_send, t_recv, t_send_rest, t_recv_rest,
    load_sems, send_sems, recv_sems, route_send_sems, route_recv_sems,
):
    zh, y, x, zl, c = [lax.axis_index(a) for a in (*PX, *PY)]
    z = zh * 2 + zl
    line = zh * 64 + y * 16
    column = x * 4 + zl * 2 + c
    me = line + column

    loads = []
    for k, (source, target) in enumerate((
        (spec_hbm, spec), (tables_hbm.at[T_Z], tables.at[T_Z]), (noise_hbm, noise),
        (tables_hbm.at[pl.ds(1, TABLES - 1)], tables.at[pl.ds(1, TABLES - 1)]),
        (twiddle_hbm, twiddle), (pairs_hbm, pairs), (rows_hbm, rows), (order_hbm, order_smem),
    )):
        load = pltpu.make_async_copy(source, target, load_sems.at[k])
        load.start()
        loads.append(load)

    def over_half(action, half):
        core = lax.rem(c + 1 - half, 2)

        def group(s, skip):
            z2 = lax.rem(z + ordered(s), 4)
            base = (z2 // 2) * 64 + lax.rem(z2, 2) * 2 + core
            ys = [lax.rem(y + ordered(lax.rem(s + t, 4)), 4) * 16 for t in range(4)]
            xs = [lax.rem(x + ordered(lax.rem(s + t, 4)), 4) * 4 for t in range(4)]
            for t in range(4):
                for u in range(4):
                    if not (skip and t == 0 and u == 0):
                        action(base + ys[t] + xs[u])

        @pl.loop(0, 4 - half)
        def _(s):
            group(s, False)

        if half:
            group(jnp.int32(3), True)

    def over_devices(action):
        over_half(action, 0)
        over_half(action, 1)

    barrier = pltpu.get_barrier_semaphore()
    over_devices(lambda d: pl.semaphore_signal(barrier, 1, device_id=d, device_id_type=LOGICAL))

    def send(source, target, send_sem, recv_sem):
        return lambda d: pltpu.make_async_remote_copy(
            source(d), target, send_sem, recv_sem, device_id=d, device_id_type=LOGICAL).start()

    def finish(ref, sem):
        pltpu.make_async_copy(ref, ref, sem).wait()

    loads[0].wait()
    for jj in range(4):
        j2lo, m2lo = divmod(jj, 2)
        starts = [(j2lo * 8 + j1) * CY + m2lo * 16 for j1 in range(8)]
        block = jnp.concatenate([spec[pl.ds(s, 16), 0:128] for s in starts], 0)
        s_send[:, jj, :] = block.T
        block = jnp.concatenate([spec[pl.ds(s, 16), 128:256] for s in starts], 0)
        n_send[0, jj, :] = block.T[0]

    row = zh * 4 + y
    on_line = jnp.logical_and(
        lax.broadcasted_iota(jnp.int32, (4, 128), 0) < 2, lax.broadcasted_iota(jnp.int32, (4, 128), 1) < 16)
    low_inside, low_line = jnp.where(row >= 4, 0, 1), jnp.where(column >= 8, 0, 1)
    low_half = jnp.where(jnp.logical_and(on_line, lax.rem(row, 4) == 0), low_line, low_inside) == 1
    lowest, highest = s_send[0], n_send[0]
    s_send[0] = jnp.where(low_half, lowest, highest)
    n_send[0] = jnp.where(low_half, highest, lowest)

    loads[1].wait()
    loads[2].wait()

    @pl.loop(0, 2)
    def _(f):
        for part in range(2):
            high, low = split(noise[f, pl.ds(part * 256, 256), :])
            out = dot_nt(tables[T_Z, 0], high) + dot_nt(tables[T_Z, 0], low) + dot_nt(tables[T_Z, 1], high)
            for ri in range(2):
                for l in range(2):
                    f_send[f, pl.ds(ri * 4 + part * 2 + l, 128, stride=8), :] = (
                        out[ri * 128:(ri + 1) * 128, l * 128:(l + 1) * 128])

    def swap_first(ref):
        first, second = ref[0, pl.ds(0, 8), :], ref[1, pl.ds(0, 8), :]
        ref[0, pl.ds(0, 8), :] = jnp.concatenate([first[:4], second[:4]], 0)
        ref[1, pl.ds(0, 8), :] = jnp.concatenate([first[4:], second[4:]], 0)

    def block_of(d):
        return pl.ds(pl.multiple_of(d * 8, 8), 8)

    swap_first(f_send)
    pl.semaphore_wait(barrier, 127)
    over_devices(send(lambda d: s_send.at[d], s_recv.at[me], send_sems.at[0], recv_sems.at[0]))
    s_recv[me] = s_send[me]
    extra = jnp.logical_and(jnp.logical_and(lax.rem(row, 4) == 0, lax.rem(column, 8) == 0), me != 0)

    @pl.when(extra)
    def _():
        pltpu.make_async_remote_copy(
            n_send.at[0], n_recv.at[(row // 4) * 2 + column // 8], send_sems.at[1], recv_sems.at[1],
            device_id=jnp.int32(0), device_id_type=LOGICAL).start()

    def send_forward(f, half):
        over_half(send(
            lambda d: f_send.at[f, block_of(d)], f_recv.at[f, block_of(me)],
            send_sems.at[2 + 2 * f + half], recv_sems.at[2 + f]), half)

    def forward_sent(f, half):
        finish(f_send.at[f, pl.ds(0, (64 - half) * 8)], send_sems.at[2 + 2 * f + half])

    send_forward(0, 0)
    send_forward(0, 1)
    send_forward(1, 0)
    send_forward(1, 1)
    for f in range(2):
        f_recv[f, block_of(me), :] = f_send[f, block_of(me), :]

    finish(s_recv.at[pl.ds(0, 127)], recv_sems.at[0])

    def arrange(plane, load):
        for j2a in range(4):
            parts = [load(2 * p_high + j2a // 2, (j2a % 2) * 2 + m2lo) for m2lo in range(2) for p_high in range(4)]
            scale[plane, j2a] = jnp.concatenate(parts, 0).T

    def received(p, jj):
        return s_recv[pl.ds(p * 16, 16), jj, :]

    @pl.when(me != 0)
    def _():
        arrange(0, received)

    @pl.when(me == 0)
    def _():
        n_recv[0] = n_send[0]
        finish(n_recv.at[pl.ds(0, 3)], recv_sems.at[1])
        lanes = lax.broadcasted_iota(jnp.int32, (128, 128), 1)
        opposite = lax.rem(8 - lax.div(lanes, 16), 8) * 16 + lax.rem(16 - lax.rem(lanes, 16), 16)
        chosen = jnp.where(lax.broadcasted_iota(jnp.int32, (128, 128), 0) == opposite, 1.0, 0.0).astype(BF16)
        for jj in range(4):
            high, low = split(s_recv[:, jj, :])
            mirrored[:, jj, :] = dot(high, chosen) + dot(low, chosen)

        @pl.loop(0, 8)
        def _(p):
            for q in range(16):
                block = mirrored[p * 16 + q]
                reversed_[p * 16 + 15 - q] = block
                wrapped[p * 16 + (16 - q) % 16] = block

        lane = lax.broadcasted_iota(jnp.int32, (16, 128), 1)

        def opposite_block(p, jj):
            j2lo, m2lo = divmod(jj, 2)

            def over_m(p2, j2):
                spots = pl.ds(p2 * 16, 16)
                ends = wrapped[spots, j2 * 2, :] if m2lo == 0 else reversed_[spots, j2 * 2 + 1, :]
                return jnp.where(lax.rem(lane, 16) == 0, ends, reversed_[spots, j2 * 2 + 1 - m2lo, :])

            ends = over_m((8 - p) % 8, 0) if j2lo == 0 else over_m(7 - p, 1)
            return jnp.where(lane < 16, ends, over_m(7 - p, 1 - j2lo))

        own = lax.broadcasted_iota(jnp.int32, (16, 128), 0)

        def plane_of(plane):
            def load(p, jj):
                block = received(p, jj) if (p >= 4) == (plane == 1) else opposite_block(p, jj)
                if p % 4 == 0 and jj < 2:
                    low, high = received(p, jj), opposite_block(p, jj)
                    if plane == 1:
                        low, high = high, low
                    on = jnp.where(own < 8, low, high)
                    if jj == 0:
                        spot = jnp.logical_and(lane == 0, own == 8 * (1 - plane))
                        on = jnp.where(spot, n_recv[(p // 4) * 2 + 1 - plane, pl.ds(0, 1), :], on)
                    block = jnp.where(lane < 16, on, block)
                return block

            return load

        for plane in range(2):
            arrange(plane, plane_of(plane))

    for load in loads[3:]:
        load.wait()
    for j2a in range(4):
        for k in range(2):
            tables_back[j2a, k] = tables[T_C + j2a, k].astype(F32).T.astype(BF16)

    def send_back(f):
        over_devices(send(
            lambda d: b_send.at[f, block_of(d)], b_recv.at[f, block_of(me)],
            send_sems.at[6 + f], recv_sems.at[4 + f]))

    @pl.loop(0, 2)
    def _(f):
        finish(f_recv.at[f, pl.ds(0, 127 * 8)], recv_sems.at[2 + f])
        for part in range(2):
            values = jnp.concatenate([
                jnp.concatenate([
                    f_recv[f, pl.ds(ri * 4 + part * 2 + l, 128, stride=8), :] for l in range(2)], 1)
                for ri in range(2)], 0)
            high, low = split(values)
            y_mid[:, part * 256:(part + 1) * 256] = (
                dot(tables[T_P, 0], high) + dot(tables[T_P, 0], low) + dot(tables[T_P, 1], high))

        @pl.loop(0, 8)
        def _(n):
            at = pl.multiple_of(n * 16, 16)
            real, imag = [], []
            for l in range(4):
                lanes = slice(l * 128, (l + 1) * 128)
                vr, vi = y_mid[pl.ds(at, 16), lanes], y_mid[pl.ds(128 + at, 16), lanes]
                wr, wi = twiddle[0, pl.ds(at, 16), lanes], twiddle[1, pl.ds(at, 16), lanes]
                real.append(vr * wr - vi * wi)
                imag.append(vr * wi + vi * wr)
            r02, r13 = real[0] + real[2], real[1] + real[3]
            i02, i13 = imag[0] + imag[2], imag[1] + imag[3]
            rd, re = real[0] - real[2], real[1] - real[3]
            id_, ie = imag[0] - imag[2], imag[1] - imag[3]
            outs = ((r02 + r13, i02 + i13), (rd + ie, id_ - re), (r02 - r13, i02 - i13), (rd - ie, id_ + re))
            for j2a, pair in enumerate(outs):
                for ri in range(2):
                    high, low = split(pair[ri])
                    v_high[j2a, pl.ds(at, 16), ri * 128:(ri + 1) * 128] = high
                    v_low[j2a, pl.ds(at, 16), ri * 128:(ri + 1) * 128] = low

        for j2a in range(4):
            high, low = v_high[j2a], v_low[j2a]
            spectral = (dot(high, tables[T_C + j2a, 0]) + dot(low, tables[T_C + j2a, 0])
                        + dot(high, tables[T_C + j2a, 1]))
            factor = scale[jnp.where(me == 0, f, 0), j2a]
            high, low = split(spectral * jnp.concatenate([factor, factor], 1))
            v_back[j2a] = (dot(high, tables_back[j2a, 0]) + dot(low, tables_back[j2a, 0])
                           + dot(high, tables_back[j2a, 1]))

        @pl.loop(0, 8)
        def _(n):
            at = pl.multiple_of(n * 16, 16)
            real = [v_back[j2a, pl.ds(at, 16), 0:128] for j2a in range(4)]
            imag = [v_back[j2a, pl.ds(at, 16), 128:256] for j2a in range(4)]
            r02, r13 = real[0] + real[2], real[1] + real[3]
            i02, i13 = imag[0] + imag[2], imag[1] + imag[3]
            rd, re = real[0] - real[2], real[1] - real[3]
            id_, ie = imag[0] - imag[2], imag[1] - imag[3]
            outs = ((r02 + r13, i02 + i13), (rd - ie, id_ + re), (r02 - r13, i02 - i13), (rd + ie, id_ - re))
            for l, (vr, vi) in enumerate(outs):
                lanes = slice(l * 128, (l + 1) * 128)
                wr, wi = twiddle[0, pl.ds(at, 16), lanes], twiddle[1, pl.ds(at, 16), lanes]
                for ri, value in enumerate((vr * wr + vi * wi, vi * wr - vr * wi)):
                    high, low = split(value)
                    z_high[pl.ds(ri * 128 + at, 16), lanes] = high
                    z_low[pl.ds(ri * 128 + at, 16), lanes] = low

        for part in range(2):
            high, low = z_high[:, part * 256:(part + 1) * 256], z_low[:, part * 256:(part + 1) * 256]
            out = dot(tables[T_PI, 0], high) + dot(tables[T_PI, 0], low) + dot(tables[T_PI, 1], high)
            for ri in range(2):
                for l in range(2):
                    half, row = jnp.where(me == 0, ri, f), jnp.where(me == 0, f, ri)
                    b_send[half, pl.ds(row * 4 + part * 2 + l, 128, stride=8), :] = (
                        out[ri * 128:(ri + 1) * 128, l * 128:(l + 1) * 128])

        @pl.when(jnp.logical_and(me == 0, f == 1))
        def _():
            send_back(0)

        @pl.when(jnp.logical_or(me != 0, f == 1))
        def _():
            send_back(f)

    for f in range(2):
        b_recv[f, block_of(me), :] = b_send[f, block_of(me), :]

    def over_column(action):
        for dx in (2, 1, 3, 0):
            for dz in (1, 0):
                for dc in (1, 0):
                    if (dx, dz, dc) != (0, 0, 0):
                        action(lax.rem(x + dx, 4) * 4 + lax.rem(zl + dz, 2) * 2 + lax.rem(c + dc, 2))

    def send_pieces(f, phase, pairs_of_refs):
        over_column(lambda g: [pltpu.make_async_remote_copy(
            source.at[g], target.at[column], route_send_sems.at[phase + k, f], route_recv_sems.at[phase + k, f],
            device_id=line + g, device_id_type=LOGICAL).start()
            for k, (source, target) in enumerate(pairs_of_refs)])
        for source, target in pairs_of_refs:
            target[column] = source[column]

    def await_pieces(f, phase, pairs_of_refs):
        for k, (_, target) in enumerate(pairs_of_refs):
            finish(target.at[pl.ds(0, 15)], route_recv_sems.at[phase + k, f])

    first_refs = [((r_send.at[0], r_recv), (r_send_rest.at[0], r_recv_rest)),
                  ((r_send.at[1], r_other), (r_send_rest.at[1], r_other_rest))]
    second_refs = [((t_send.at[f], t_recv.at[f]), (t_send_rest.at[f], t_recv_rest.at[f])) for f in range(2)]

    fewer = lax.broadcasted_iota(jnp.int32, (32, 128), 1) < 64

    for f in range(2):
        finish(b_recv.at[f, pl.ds(0, 127 * 8)], recv_sems.at[4 + f])
        for l in range(4):
            cells = pl.ds(l * 128, 128)
            values = jnp.concatenate(
                [b_recv[f, pl.ds(ri * 4 + l, 128, stride=8), :].T for ri in range(2)], 1)
            high, low = split(values)
            fields = dot(high, tables[T_U, 0]) + dot(low, tables[T_U, 0]) + dot(high, tables[T_U, 1])
            modulus = jnp.exp(0.5 * fields)
            modulus_ref[f, cells, :] = modulus
            high, low = split(modulus)
            high, low = split(dot(high, pairs[...]) + dot(low, pairs[...]))
            g_high[cells, :] = high
            g_low[cells, :] = low
        coarse = dot(rows[...], g_high[...]) + dot(rows[...], g_low[...])
        r_send[f] = coarse[0:128, 0:128].reshape(16, 8, 128)
        r_send_rest[f] = jnp.where(fewer, coarse[128:160, 128:256], coarse[160:192, 128:256]).reshape(16, 2, 128)
        send_pieces(f, 0, first_refs[f])

    for f in range(2):
        await_pieces(f, 0, first_refs[f])
        (_, held), (_, held_rest) = first_refs[f]

        @pl.loop(0, 16)
        def _(g):
            t_send[f, g] = held[order_smem[0, g]]
            second, third = held_rest[order_smem[1, g]], held_rest[order_smem[2, g]]
            t_send_rest[f, g] = jnp.where(fewer[0:2], second, third)

        send_pieces(f, 2, second_refs[f])

    for f in range(2):
        await_pieces(f, 2, second_refs[f])
        fine_ref[f] = t_recv[f]
        rest_ref[f] = t_recv_rest[f]

    finish(s_send.at[pl.ds(0, 127)], send_sems.at[0])

    @pl.when(extra)
    def _():
        finish(n_send.at[0], send_sems.at[1])

    for f in range(2):
        finish(b_send.at[f, pl.ds(0, 127 * 8)], send_sems.at[6 + f])
        for k, (whole, rest) in enumerate(((r_send, r_send_rest), (t_send, t_send_rest))):
            finish(whole.at[f, pl.ds(0, 15)], route_send_sems.at[2 * k, f])
            finish(rest.at[f, pl.ds(0, 15)], route_send_sems.at[2 * k + 1, f])
    for f in range(2):
        for half in range(2):
            forward_sent(f, half)


def finisher(modulus_ref, fine_ref, rest_ref, modulus_hbm, one_ref, two_ref, three_ref, sem):
    store = pltpu.make_async_copy(modulus_ref, modulus_hbm, sem)
    store.start()
    for f in range(2):
        one_ref[pl.ds(f * 128, 128), :] = fine_ref[f].reshape(128, 128)
        rest = rest_ref[f]
        two_ref[pl.ds(f * 32, 32), :] = rest.reshape(32, 128)[:, 0:64]
        three_ref[pl.ds(f * 8, 8), :] = rest[0:8, 0, 64:96]
    store.wait()


def on_device(white_noise, spectrum, group_table):
    tables, twiddle, pairs, rows = build_tables()
    hbm = pl.BlockSpec(memory_space=pltpu.HBM)
    vmem = pl.BlockSpec(memory_space=pltpu.VMEM)
    modulus_shape = jax.ShapeDtypeStruct((2, CELLS, NZ), F32)
    modulus, fine, rest = pl.pallas_call(
        kernel,
        out_shape=(pltpu.VMEM((2, CELLS, NZ), F32), pltpu.VMEM((2, 16, 8, 128), F32), pltpu.VMEM((2, 16, 2, 128), F32)),
        in_specs=[hbm] * 7,
        out_specs=(vmem, vmem, vmem),
        scratch_shapes=[
            pltpu.SMEM((3, 16), jnp.int32),
            pltpu.VMEM((2, CELLS, NZ), F32),
            pltpu.VMEM((CELLS, NZ), F32),
            pltpu.VMEM((TABLES, 2, 256, 256), BF16),
            pltpu.VMEM((2, 128, CELLS), F32),
            pltpu.VMEM((NZ, 256), BF16),
            pltpu.VMEM((192, CELLS), BF16),
            pltpu.VMEM((4, 2, 256, 256), BF16),
            pltpu.VMEM((128, 4, 128), F32),
            pltpu.VMEM((128, 4, 128), F32),
            pltpu.VMEM((1, 4, 128), F32),
            pltpu.VMEM((4, 4, 128), F32),
            *[pltpu.VMEM((128, 4, 128), F32)] * 3,
            pltpu.VMEM((2, 4, 128, 128), F32),
            pltpu.VMEM((2, 1024, 128), F32),
            pltpu.VMEM((2, 1024, 128), F32),
            pltpu.VMEM((2, 1024, 128), F32),
            pltpu.VMEM((2, 1024, 128), F32),
            pltpu.VMEM((256, CELLS), F32),
            pltpu.VMEM((4, 128, 256), BF16),
            pltpu.VMEM((4, 128, 256), BF16),
            pltpu.VMEM((4, 128, 256), F32),
            pltpu.VMEM((256, CELLS), BF16),
            pltpu.VMEM((256, CELLS), BF16),
            pltpu.VMEM((CELLS, 256), BF16),
            pltpu.VMEM((CELLS, 256), BF16),
            *[pltpu.VMEM((*count, 16, size, 128), F32) for size in (8, 2) for count in ((2,), (), ())],
            *[pltpu.VMEM((2, 16, size, 128), F32) for size in (8, 8, 2, 2)],
            pltpu.SemaphoreType.DMA((8,)),
            pltpu.SemaphoreType.DMA((8,)),
            pltpu.SemaphoreType.DMA((6,)),
            pltpu.SemaphoreType.DMA((4, 2)),
            pltpu.SemaphoreType.DMA((4, 2)),
        ],
        compiler_params=pltpu.CompilerParams(
            collective_id=0, has_side_effects=True, vmem_limit_bytes=60000000),
        name="moduli",
    )(
        white_noise.reshape(2, CELLS, NZ), spectrum.reshape(CELLS, NZ), group_table,
        jnp.asarray(tables), jnp.asarray(twiddle), jnp.asarray(pairs), jnp.asarray(rows),
    )
    modulus, one, two, three = pl.pallas_call(
        finisher,
        out_shape=(
            modulus_shape,
            jax.ShapeDtypeStruct((256, 128), F32),
            jax.ShapeDtypeStruct((64, 64), F32),
            jax.ShapeDtypeStruct((16, 32), F32),
        ),
        in_specs=[vmem, vmem, vmem],
        out_specs=(hbm, vmem, vmem, vmem),
        scratch_shapes=[pltpu.SemaphoreType.DMA],
        compiler_params=pltpu.CompilerParams(vmem_limit_bytes=4 << 20),
        name="levels",
    )(modulus, fine, rest)
    return (
        modulus.reshape(2, CX, CY, NZ),
        one.reshape(2, 8, 16, 128),
        two.reshape(2, 4, 8, 64),
        three.reshape(2, 2, 4, 32),
    )


def solution(mesh):
    split_mesh = Mesh(mesh.devices.reshape(2, 4, 4, 2, 2), (*PX, *PY))
    whole = P(None, PX, PY, None)
    return jax.shard_map(
        on_device,
        mesh=split_mesh,
        in_specs=(whole, P(PX, PY, None), P()),
        out_specs=(whole, whole, whole, whole),
        check_vma=False,
    )
```

```python
import functools

import jax
import jax.numpy as jnp
import ml_dtypes
import numpy as np
from jax import lax
from jax.experimental import pallas as pl
from jax.experimental.pallas import tpu as pltpu
from jax.sharding import Mesh
from jax.sharding import PartitionSpec as P

PX = ("px_0", "px_1")
PY = ("py_0", "py_1", "py_2")
F32 = jnp.float32
BF16 = jnp.bfloat16
LOGICAL = pl.DeviceIdType.LOGICAL

NX, NY, NZ = 128, 512, 256
CX, CY = 16, 32
CELLS = CX * CY
T_Z, T_P, T_C, T_PI, T_U, TABLES = 0, 1, 2, 6, 7, 8


def wave(products, length, sign):
    angles = 2.0 * np.pi * (products % length) / length
    return np.cos(angles), sign * np.sin(angles)


def applied_left(real, imag):
    return np.block([[real, -imag], [imag, real]])


def build_tables():
    spots = np.arange(128)
    z = np.arange(NZ)
    p, q = spots // 16, spots % 16
    j1, m1 = spots // 16, spots % 16
    tables = np.zeros((TABLES, 256, 256))
    cos_z, sin_z = wave(spots[:, None] * z[None, :], NZ, -1.0)
    sin_z[0] = (-1.0) ** z
    tables[T_Z] = np.concatenate([cos_z, sin_z], 0)
    weight = np.where(spots == 0, 1.0, 2.0)[:, None] / float(NX * NY * NZ)
    tables[T_U] = np.concatenate([cos_z * weight, sin_z * weight], 0)
    outer = 2 * p[None, :] * j1[:, None] + q[None, :] * m1[:, None]
    tables[T_P] = applied_left(*wave(outer, 16, -1.0))
    tables[T_PI] = applied_left(*wave(outer.T, 16, 1.0))
    low, b = spots // 32, spots % 32
    half, j2b, q2 = spots // 64, (spots // 16) % 4, spots % 16
    m2 = 2 * q2 + half
    for j2a in range(4):
        inner = 2 * low[:, None] * j2a + 8 * low[:, None] * j2b[None, :] + b[:, None] * m2[None, :]
        tables[T_C + j2a] = applied_left(*wave(inner.T, 32, -1.0)).T
    cell_a, cell_b = np.arange(CELLS) // CY, np.arange(CELLS) % CY
    middle = 4 * cell_a[None, :] * j1[:, None] + cell_b[None, :] * m1[:, None]
    twiddle = np.stack(wave(middle, 512, -1.0)).astype(np.float32)
    high = tables.astype(np.float32).astype(ml_dtypes.bfloat16)
    rest = (tables - high.astype(np.float64)).astype(np.float32).astype(ml_dtypes.bfloat16)
    pairs = np.zeros((NZ, 256))
    pairs[z, z // 2] = 0.5
    pairs[z, 128 + z // 4] = 0.25
    pairs[z, 192 + z // 8] = 0.125
    rows = np.zeros((192, CELLS))
    for cell in range(CELLS):
        a, b = divmod(cell, CY)
        rows[(a // 2) * 16 + b // 2, cell] = 0.25
        rows[128 + (a // 4) * 8 + b // 4, cell] = 1.0 / 16
        rows[160 + 2 * ((a // 8) * 4 + b // 8), cell] = 1.0 / 64
    exact = ml_dtypes.bfloat16
    return np.stack([high, rest], 1), twiddle, pairs.astype(exact), rows.astype(exact)


def dot(left, right):
    return jnp.dot(left, right, preferred_element_type=F32)


def dot_nt(left, right):
    return lax.dot_general(left, right, (((1,), (1,)), ((), ())), preferred_element_type=F32)


def split(values):
    high = values.astype(BF16)
    return high, (values - high.astype(F32)).astype(BF16)


def ordered(index):
    return lax.rem(2 - index + 3 * (index // 2) + 2 * (index // 3) + 4, 4)


def kernel(
    noise_hbm, spec_hbm, order_hbm, tables_hbm, twiddle_hbm, pairs_hbm, rows_hbm,
    modulus_ref, fine_ref, rest_ref,
    order_smem, noise, spec, tables, twiddle, pairs, rows,
    tables_back, s_send, s_recv, n_send, n_recv, mirrored, reversed_, wrapped, scale, f_send, f_recv, b_send, b_recv,
    y_mid, v_high, v_low, v_back, z_high, z_low, w_high, w_low, g_high, g_low,
    r_send, r_recv, r_other, r_send_rest, r_recv_rest, r_other_rest, t_send, t_recv, t_send_rest, t_recv_rest,
    load_sems, send_sems, recv_sems, route_send_sems, route_recv_sems,
):
    zh, y, x, zl, c = [lax.axis_index(a) for a in (*PX, *PY)]
    z = zh * 2 + zl
    line = zh * 64 + y * 16
    column = x * 4 + zl * 2 + c
    me = line + column

    loads = []
    for k, (source, target) in enumerate((
        (spec_hbm, spec), (tables_hbm.at[T_Z], tables.at[T_Z]), (noise_hbm, noise),
        (tables_hbm.at[pl.ds(1, TABLES - 1)], tables.at[pl.ds(1, TABLES - 1)]),
        (twiddle_hbm, twiddle), (pairs_hbm, pairs), (rows_hbm, rows), (order_hbm, order_smem),
    )):
        load = pltpu.make_async_copy(source, target, load_sems.at[k])
        load.start()
        loads.append(load)

    def over_half(action, half):
        core = lax.rem(c + 1 - half, 2)

        def group(s, skip):
            z2 = lax.rem(z + ordered(s), 4)
            base = (z2 // 2) * 64 + lax.rem(z2, 2) * 2 + core
            ys = [lax.rem(y + ordered(lax.rem(s + t, 4)), 4) * 16 for t in range(4)]
            xs = [lax.rem(x + ordered(lax.rem(s + t, 4)), 4) * 4 for t in range(4)]
            for t in range(4):
                for u in range(4):
                    if not (skip and t == 0 and u == 0):
                        action(base + ys[t] + xs[u])

        @pl.loop(0, 4 - half)
        def _(s):
            group(s, False)

        if half:
            group(jnp.int32(3), True)

    def over_devices(action):
        over_half(action, 0)
        over_half(action, 1)

    barrier = pltpu.get_barrier_semaphore()
    over_devices(lambda d: pl.semaphore_signal(barrier, 1, device_id=d, device_id_type=LOGICAL))

    def send(source, target, send_sem, recv_sem):
        return lambda d: pltpu.make_async_remote_copy(
            source(d), target, send_sem, recv_sem, device_id=d, device_id_type=LOGICAL).start()

    def finish(ref, sem):
        pltpu.make_async_copy(ref, ref, sem).wait()

    loads[0].wait()
    for jj in range(4):
        j2lo, m2lo = divmod(jj, 2)
        starts = [(j2lo * 8 + j1) * CY + m2lo * 16 for j1 in range(8)]
        block = jnp.concatenate([spec[pl.ds(s, 16), 0:128] for s in starts], 0)
        s_send[:, jj, :] = block.T
        block = jnp.concatenate([spec[pl.ds(s, 16), 128:256] for s in starts], 0)
        n_send[0, jj, :] = block.T[0]

    row = zh * 4 + y
    on_line = jnp.logical_and(
        lax.broadcasted_iota(jnp.int32, (4, 128), 0) < 2, lax.broadcasted_iota(jnp.int32, (4, 128), 1) < 16)
    low_inside, low_line = jnp.where(row >= 4, 0, 1), jnp.where(column >= 8, 0, 1)
    low_half = jnp.where(jnp.logical_and(on_line, lax.rem(row, 4) == 0), low_line, low_inside) == 1
    lowest, highest = s_send[0], n_send[0]
    s_send[0] = jnp.where(low_half, lowest, highest)
    n_send[0] = jnp.where(low_half, highest, lowest)

    loads[1].wait()
    loads[2].wait()

    @pl.loop(0, 2)
    def _(f):
        for part in range(2):
            high, low = split(noise[f, pl.ds(part * 256, 256), :])
            out = dot_nt(tables[T_Z, 0], high) + dot_nt(tables[T_Z, 0], low) + dot_nt(tables[T_Z, 1], high)
            for ri in range(2):
                for l in range(2):
                    f_send[f, pl.ds(ri * 4 + part * 2 + l, 128, stride=8), :] = (
                        out[ri * 128:(ri + 1) * 128, l * 128:(l + 1) * 128])

    def swap_first(ref):
        first, second = ref[0, pl.ds(0, 8), :], ref[1, pl.ds(0, 8), :]
        ref[0, pl.ds(0, 8), :] = jnp.concatenate([first[:4], second[:4]], 0)
        ref[1, pl.ds(0, 8), :] = jnp.concatenate([first[4:], second[4:]], 0)

    def block_of(d):
        return pl.ds(pl.multiple_of(d * 8, 8), 8)

    swap_first(f_send)
    pl.semaphore_wait(barrier, 127)
    over_devices(send(lambda d: s_send.at[d], s_recv.at[me], send_sems.at[0], recv_sems.at[0]))
    s_recv[me] = s_send[me]
    extra = jnp.logical_and(jnp.logical_and(lax.rem(row, 4) == 0, lax.rem(column, 8) == 0), me != 0)

    @pl.when(extra)
    def _():
        pltpu.make_async_remote_copy(
            n_send.at[0], n_recv.at[(row // 4) * 2 + column // 8], send_sems.at[1], recv_sems.at[1],
            device_id=jnp.int32(0), device_id_type=LOGICAL).start()

    def send_forward(f, half):
        over_half(send(
            lambda d: f_send.at[f, block_of(d)], f_recv.at[f, block_of(me)],
            send_sems.at[2 + 2 * f + half], recv_sems.at[2 + f]), half)

    def forward_sent(f, half):
        finish(f_send.at[f, pl.ds(0, (64 - half) * 8)], send_sems.at[2 + 2 * f + half])

    send_forward(0, 0)
    send_forward(0, 1)
    for f in range(2):
        f_recv[f, block_of(me), :] = f_send[f, block_of(me), :]

    finish(s_recv.at[pl.ds(0, 127)], recv_sems.at[0])

    def arrange(plane, load):
        for j2a in range(4):
            parts = [load(2 * p_high + j2a // 2, (j2a % 2) * 2 + m2lo) for m2lo in range(2) for p_high in range(4)]
            scale[plane, j2a] = jnp.concatenate(parts, 0).T

    def received(p, jj):
        return s_recv[pl.ds(p * 16, 16), jj, :]

    @pl.when(me != 0)
    def _():
        arrange(0, received)

    @pl.when(me == 0)
    def _():
        n_recv[0] = n_send[0]
        finish(n_recv.at[pl.ds(0, 3)], recv_sems.at[1])
        lanes = lax.broadcasted_iota(jnp.int32, (128, 128), 1)
        opposite = lax.rem(8 - lax.div(lanes, 16), 8) * 16 + lax.rem(16 - lax.rem(lanes, 16), 16)
        chosen = jnp.where(lax.broadcasted_iota(jnp.int32, (128, 128), 0) == opposite, 1.0, 0.0).astype(BF16)
        for jj in range(4):
            high, low = split(s_recv[:, jj, :])
            mirrored[:, jj, :] = dot(high, chosen) + dot(low, chosen)

        @pl.loop(0, 8)
        def _(p):
            for q in range(16):
                block = mirrored[p * 16 + q]
                reversed_[p * 16 + 15 - q] = block
                wrapped[p * 16 + (16 - q) % 16] = block

        lane = lax.broadcasted_iota(jnp.int32, (16, 128), 1)

        def opposite_block(p, jj):
            j2lo, m2lo = divmod(jj, 2)

            def over_m(p2, j2):
                spots = pl.ds(p2 * 16, 16)
                ends = wrapped[spots, j2 * 2, :] if m2lo == 0 else reversed_[spots, j2 * 2 + 1, :]
                return jnp.where(lax.rem(lane, 16) == 0, ends, reversed_[spots, j2 * 2 + 1 - m2lo, :])

            ends = over_m((8 - p) % 8, 0) if j2lo == 0 else over_m(7 - p, 1)
            return jnp.where(lane < 16, ends, over_m(7 - p, 1 - j2lo))

        own = lax.broadcasted_iota(jnp.int32, (16, 128), 0)

        def plane_of(plane):
            def load(p, jj):
                block = received(p, jj) if (p >= 4) == (plane == 1) else opposite_block(p, jj)
                if p % 4 == 0 and jj < 2:
                    low, high = received(p, jj), opposite_block(p, jj)
                    if plane == 1:
                        low, high = high, low
                    on = jnp.where(own < 8, low, high)
                    if jj == 0:
                        spot = jnp.logical_and(lane == 0, own == 8 * (1 - plane))
                        on = jnp.where(spot, n_recv[(p // 4) * 2 + 1 - plane, pl.ds(0, 1), :], on)
                    block = jnp.where(lane < 16, on, block)
                return block

            return load

        for plane in range(2):
            arrange(plane, plane_of(plane))

    send_forward(1, 0)
    send_forward(1, 1)
    for load in loads[3:]:
        load.wait()
    for j2a in range(4):
        for k in range(2):
            tables_back[j2a, k] = tables[T_C + j2a, k].astype(F32).T.astype(BF16)

    def send_back(f):
        over_devices(send(
            lambda d: b_send.at[f, block_of(d)], b_recv.at[f, block_of(me)],
            send_sems.at[6 + f], recv_sems.at[4 + f]))

    @pl.loop(0, 2)
    def _(f):
        finish(f_recv.at[f, pl.ds(0, 127 * 8)], recv_sems.at[2 + f])
        for part in range(2):
            values = jnp.concatenate([
                jnp.concatenate([
                    f_recv[f, pl.ds(ri * 4 + part * 2 + l, 128, stride=8), :] for l in range(2)], 1)
                for ri in range(2)], 0)
            high, low = split(values)
            y_mid[:, part * 256:(part + 1) * 256] = (
                dot(tables[T_P, 0], high) + dot(tables[T_P, 0], low) + dot(tables[T_P, 1], high))

        @pl.loop(0, 8)
        def _(n):
            at = pl.multiple_of(n * 16, 16)
            real, imag = [], []
            for l in range(4):
                lanes = slice(l * 128, (l + 1) * 128)
                vr, vi = y_mid[pl.ds(at, 16), lanes], y_mid[pl.ds(128 + at, 16), lanes]
                wr, wi = twiddle[0, pl.ds(at, 16), lanes], twiddle[1, pl.ds(at, 16), lanes]
                real.append(vr * wr - vi * wi)
                imag.append(vr * wi + vi * wr)
            r02, r13 = real[0] + real[2], real[1] + real[3]
            i02, i13 = imag[0] + imag[2], imag[1] + imag[3]
            rd, re = real[0] - real[2], real[1] - real[3]
            id_, ie = imag[0] - imag[2], imag[1] - imag[3]
            outs = ((r02 + r13, i02 + i13), (rd + ie, id_ - re), (r02 - r13, i02 - i13), (rd - ie, id_ + re))
            for j2a, pair in enumerate(outs):
                for ri in range(2):
                    high, low = split(pair[ri])
                    v_high[j2a, pl.ds(at, 16), ri * 128:(ri + 1) * 128] = high
                    v_low[j2a, pl.ds(at, 16), ri * 128:(ri + 1) * 128] = low

        for j2a in range(4):
            high, low = v_high[j2a], v_low[j2a]
            spectral = (dot(high, tables[T_C + j2a, 0]) + dot(low, tables[T_C + j2a, 0])
                        + dot(high, tables[T_C + j2a, 1]))
            factor = scale[jnp.where(me == 0, f, 0), j2a]
            high, low = split(spectral * jnp.concatenate([factor, factor], 1))
            v_back[j2a] = (dot(high, tables_back[j2a, 0]) + dot(low, tables_back[j2a, 0])
                           + dot(high, tables_back[j2a, 1]))

        @pl.loop(0, 8)
        def _(n):
            at = pl.multiple_of(n * 16, 16)
            real = [v_back[j2a, pl.ds(at, 16), 0:128] for j2a in range(4)]
            imag = [v_back[j2a, pl.ds(at, 16), 128:256] for j2a in range(4)]
            r02, r13 = real[0] + real[2], real[1] + real[3]
            i02, i13 = imag[0] + imag[2], imag[1] + imag[3]
            rd, re = real[0] - real[2], real[1] - real[3]
            id_, ie = imag[0] - imag[2], imag[1] - imag[3]
            outs = ((r02 + r13, i02 + i13), (rd - ie, id_ + re), (r02 - r13, i02 - i13), (rd + ie, id_ - re))
            for l, (vr, vi) in enumerate(outs):
                lanes = slice(l * 128, (l + 1) * 128)
                wr, wi = twiddle[0, pl.ds(at, 16), lanes], twiddle[1, pl.ds(at, 16), lanes]
                for ri, value in enumerate((vr * wr + vi * wi, vi * wr - vr * wi)):
                    high, low = split(value)
                    z_high[pl.ds(ri * 128 + at, 16), lanes] = high
                    z_low[pl.ds(ri * 128 + at, 16), lanes] = low

        for part in range(2):
            high, low = z_high[:, part * 256:(part + 1) * 256], z_low[:, part * 256:(part + 1) * 256]
            out = dot(tables[T_PI, 0], high) + dot(tables[T_PI, 0], low) + dot(tables[T_PI, 1], high)
            for ri in range(2):
                for l in range(2):
                    half, row = jnp.where(me == 0, ri, f), jnp.where(me == 0, f, ri)
                    b_send[half, pl.ds(row * 4 + part * 2 + l, 128, stride=8), :] = (
                        out[ri * 128:(ri + 1) * 128, l * 128:(l + 1) * 128])

        @pl.when(jnp.logical_and(me == 0, f == 1))
        def _():
            send_back(0)

        @pl.when(jnp.logical_or(me != 0, f == 1))
        def _():
            send_back(f)

    for f in range(2):
        b_recv[f, block_of(me), :] = b_send[f, block_of(me), :]

    def over_column(action):
        for dx in (2, 1, 3, 0):
            for dz in (1, 0):
                for dc in (1, 0):
                    if (dx, dz, dc) != (0, 0, 0):
                        action(lax.rem(x + dx, 4) * 4 + lax.rem(zl + dz, 2) * 2 + lax.rem(c + dc, 2))

    def send_pieces(f, phase, pairs_of_refs):
        over_column(lambda g: [pltpu.make_async_remote_copy(
            source.at[g], target.at[column], route_send_sems.at[phase + k, f], route_recv_sems.at[phase + k, f],
            device_id=line + g, device_id_type=LOGICAL).start()
            for k, (source, target) in enumerate(pairs_of_refs)])
        for source, target in pairs_of_refs:
            target[column] = source[column]

    def await_pieces(f, phase, pairs_of_refs):
        for k, (_, target) in enumerate(pairs_of_refs):
            finish(target.at[pl.ds(0, 15)], route_recv_sems.at[phase + k, f])

    first_refs = [((r_send.at[0], r_recv), (r_send_rest.at[0], r_recv_rest)),
                  ((r_send.at[1], r_other), (r_send_rest.at[1], r_other_rest))]
    second_refs = [((t_send.at[f], t_recv.at[f]), (t_send_rest.at[f], t_recv_rest.at[f])) for f in range(2)]

    fewer = lax.broadcasted_iota(jnp.int32, (32, 128), 1) < 64

    for f in range(2):
        finish(b_recv.at[f, pl.ds(0, 127 * 8)], recv_sems.at[4 + f])
        for l in range(4):
            cells = pl.ds(l * 128, 128)
            for ri in range(2):
                high, low = split(b_recv[f, pl.ds(ri * 4 + l, 128, stride=8), :].T)
                w_high[cells, ri * 128:(ri + 1) * 128] = high
                w_low[cells, ri * 128:(ri + 1) * 128] = low
        for part in range(2):
            cells = pl.ds(part * 256, 256)
            high, low = w_high[cells, :], w_low[cells, :]
            fields = dot(high, tables[T_U, 0]) + dot(low, tables[T_U, 0]) + dot(high, tables[T_U, 1])
            modulus = jnp.exp(0.5 * fields)
            modulus_ref[f, cells, :] = modulus
            high, low = split(modulus)
            high, low = split(dot(high, pairs[...]) + dot(low, pairs[...]))
            g_high[cells, :] = high
            g_low[cells, :] = low
        coarse = dot(rows[...], g_high[...]) + dot(rows[...], g_low[...])
        r_send[f] = coarse[0:128, 0:128].reshape(16, 8, 128)
        r_send_rest[f] = jnp.where(fewer, coarse[128:160, 128:256], coarse[160:192, 128:256]).reshape(16, 2, 128)
        send_pieces(f, 0, first_refs[f])

    for f in range(2):
        await_pieces(f, 0, first_refs[f])
        (_, held), (_, held_rest) = first_refs[f]

        @pl.loop(0, 16)
        def _(g):
            t_send[f, g] = held[order_smem[0, g]]
            second, third = held_rest[order_smem[1, g]], held_rest[order_smem[2, g]]
            t_send_rest[f, g] = jnp.where(fewer[0:2], second, third)

        send_pieces(f, 2, second_refs[f])

    for f in range(2):
        await_pieces(f, 2, second_refs[f])
        fine_ref[f] = t_recv[f]
        rest_ref[f] = t_recv_rest[f]

    finish(s_send.at[pl.ds(0, 127)], send_sems.at[0])

    @pl.when(extra)
    def _():
        finish(n_send.at[0], send_sems.at[1])

    for f in range(2):
        finish(b_send.at[f, pl.ds(0, 127 * 8)], send_sems.at[6 + f])
        for k, (whole, rest) in enumerate(((r_send, r_send_rest), (t_send, t_send_rest))):
            finish(whole.at[f, pl.ds(0, 15)], route_send_sems.at[2 * k, f])
            finish(rest.at[f, pl.ds(0, 15)], route_send_sems.at[2 * k + 1, f])
    for f in range(2):
        for half in range(2):
            forward_sent(f, half)


def finisher(modulus_ref, fine_ref, rest_ref, modulus_hbm, one_hbm, two_hbm, three_hbm, two, three, sems):
    stores = [
        pltpu.make_async_copy(source, target, sems.at[k]) for k, (source, target) in enumerate((
            (modulus_ref, modulus_hbm), (fine_ref, one_hbm), (two, two_hbm), (three, three_hbm)))]
    stores[0].start()
    stores[1].start()
    for f in range(2):
        rest = rest_ref[f]
        two[pl.ds(f * 32, 32), :] = rest.reshape(32, 128)[:, 0:64]
        three[pl.ds(f * 8, 8), :] = rest[0:8, 0, 64:96]
    stores[2].start()
    stores[3].start()
    for store in stores:
        store.wait()


def on_device(white_noise, spectrum, group_table):
    tables, twiddle, pairs, rows = build_tables()
    hbm = pl.BlockSpec(memory_space=pltpu.HBM)
    vmem = pl.BlockSpec(memory_space=pltpu.VMEM)
    modulus_shape = jax.ShapeDtypeStruct((2, CELLS, NZ), F32)
    modulus, fine, rest = pl.pallas_call(
        kernel,
        out_shape=(pltpu.VMEM((2, CELLS, NZ), F32), pltpu.VMEM((2, 16, 8, 128), F32), pltpu.VMEM((2, 16, 2, 128), F32)),
        in_specs=[hbm] * 7,
        out_specs=(vmem, vmem, vmem),
        scratch_shapes=[
            pltpu.SMEM((3, 16), jnp.int32),
            pltpu.VMEM((2, CELLS, NZ), F32),
            pltpu.VMEM((CELLS, NZ), F32),
            pltpu.VMEM((TABLES, 2, 256, 256), BF16),
            pltpu.VMEM((2, 128, CELLS), F32),
            pltpu.VMEM((NZ, 256), BF16),
            pltpu.VMEM((192, CELLS), BF16),
            pltpu.VMEM((4, 2, 256, 256), BF16),
            pltpu.VMEM((128, 4, 128), F32),
            pltpu.VMEM((128, 4, 128), F32),
            pltpu.VMEM((1, 4, 128), F32),
            pltpu.VMEM((4, 4, 128), F32),
            *[pltpu.VMEM((128, 4, 128), F32)] * 3,
            pltpu.VMEM((2, 4, 128, 128), F32),
            pltpu.VMEM((2, 1024, 128), F32),
            pltpu.VMEM((2, 1024, 128), F32),
            pltpu.VMEM((2, 1024, 128), F32),
            pltpu.VMEM((2, 1024, 128), F32),
            pltpu.VMEM((256, CELLS), F32),
            pltpu.VMEM((4, 128, 256), BF16),
            pltpu.VMEM((4, 128, 256), BF16),
            pltpu.VMEM((4, 128, 256), F32),
            pltpu.VMEM((256, CELLS), BF16),
            pltpu.VMEM((256, CELLS), BF16),
            *[pltpu.VMEM((CELLS, 256), BF16)] * 4,
            *[pltpu.VMEM((*count, 16, size, 128), F32) for size in (8, 2) for count in ((2,), (), ())],
            *[pltpu.VMEM((2, 16, size, 128), F32) for size in (8, 8, 2, 2)],
            pltpu.SemaphoreType.DMA((8,)),
            pltpu.SemaphoreType.DMA((8,)),
            pltpu.SemaphoreType.DMA((6,)),
            pltpu.SemaphoreType.DMA((4, 2)),
            pltpu.SemaphoreType.DMA((4, 2)),
        ],
        compiler_params=pltpu.CompilerParams(
            collective_id=0, has_side_effects=True, vmem_limit_bytes=60000000),
        name="moduli",
    )(
        white_noise.reshape(2, CELLS, NZ), spectrum.reshape(CELLS, NZ), group_table,
        jnp.asarray(tables), jnp.asarray(twiddle), jnp.asarray(pairs), jnp.asarray(rows),
    )
    modulus, one, two, three = pl.pallas_call(
        finisher,
        out_shape=(
            modulus_shape,
            jax.ShapeDtypeStruct((2, 16, 8, 128), F32),
            jax.ShapeDtypeStruct((64, 64), F32),
            jax.ShapeDtypeStruct((16, 32), F32),
        ),
        in_specs=[vmem, vmem, vmem],
        out_specs=(hbm, hbm, hbm, hbm),
        scratch_shapes=[pltpu.VMEM((64, 64), F32), pltpu.VMEM((16, 32), F32), pltpu.SemaphoreType.DMA((4,))],
        compiler_params=pltpu.CompilerParams(vmem_limit_bytes=4 << 20),
        name="levels",
    )(modulus, fine, rest)
    return (
        modulus.reshape(2, CX, CY, NZ),
        one.reshape(2, 8, 16, 128),
        two.reshape(2, 4, 8, 64),
        three.reshape(2, 2, 4, 32),
    )


def solution(mesh):
    split_mesh = Mesh(mesh.devices.reshape(2, 4, 4, 2, 2), (*PX, *PY))
    whole = P(None, PX, PY, None)
    return jax.shard_map(
        on_device,
        mesh=split_mesh,
        in_specs=(whole, P(PX, PY, None), P()),
        out_specs=(whole, whole, whole, whole),
        check_vma=False,
    )
```

```python
import functools

import jax
import jax.numpy as jnp
import ml_dtypes
import numpy as np
from jax import lax
from jax.experimental import pallas as pl
from jax.experimental.pallas import tpu as pltpu
from jax.sharding import Mesh
from jax.sharding import PartitionSpec as P

PX = ("px_0", "px_1")
PY = ("py_0", "py_1", "py_2")
F32 = jnp.float32
BF16 = jnp.bfloat16
LOGICAL = pl.DeviceIdType.LOGICAL

NX, NY, NZ = 128, 512, 256
CX, CY = 16, 32
CELLS = CX * CY
T_Z, T_P, T_C, T_PI, T_U, TABLES = 0, 1, 2, 6, 7, 8


def wave(products, length, sign):
    angles = 2.0 * np.pi * (products % length) / length
    return np.cos(angles), sign * np.sin(angles)


def applied_left(real, imag):
    return np.block([[real, -imag], [imag, real]])


def build_tables():
    spots = np.arange(128)
    z = np.arange(NZ)
    p, q = spots // 16, spots % 16
    j1, m1 = spots // 16, spots % 16
    tables = np.zeros((TABLES, 256, 256))
    cos_z, sin_z = wave(spots[:, None] * z[None, :], NZ, -1.0)
    sin_z[0] = (-1.0) ** z
    tables[T_Z] = np.concatenate([cos_z, sin_z], 0)
    weight = np.where(spots == 0, 1.0, 2.0)[:, None] / float(NX * NY * NZ)
    tables[T_U] = np.concatenate([cos_z * weight, sin_z * weight], 0)
    outer = 2 * p[None, :] * j1[:, None] + q[None, :] * m1[:, None]
    tables[T_P] = applied_left(*wave(outer, 16, -1.0))
    tables[T_PI] = applied_left(*wave(outer.T, 16, 1.0))
    low, b = spots // 32, spots % 32
    half, j2b, q2 = spots // 64, (spots // 16) % 4, spots % 16
    m2 = 2 * q2 + half
    for j2a in range(4):
        inner = 2 * low[:, None] * j2a + 8 * low[:, None] * j2b[None, :] + b[:, None] * m2[None, :]
        tables[T_C + j2a] = applied_left(*wave(inner.T, 32, -1.0)).T
    cell_a, cell_b = np.arange(CELLS) // CY, np.arange(CELLS) % CY
    middle = 4 * cell_a[None, :] * j1[:, None] + cell_b[None, :] * m1[:, None]
    twiddle = np.stack(wave(middle, 512, -1.0)).astype(np.float32)
    high = tables.astype(np.float32).astype(ml_dtypes.bfloat16)
    rest = (tables - high.astype(np.float64)).astype(np.float32).astype(ml_dtypes.bfloat16)
    pairs = np.zeros((NZ, 256))
    pairs[z, z // 2] = 0.5
    pairs[z, 128 + z // 4] = 0.25
    pairs[z, 192 + z // 8] = 0.125
    rows = np.zeros((192, CELLS))
    for cell in range(CELLS):
        a, b = divmod(cell, CY)
        rows[(a // 2) * 16 + b // 2, cell] = 0.25
        rows[128 + (a // 4) * 8 + b // 4, cell] = 1.0 / 16
        rows[160 + 2 * ((a // 8) * 4 + b // 8), cell] = 1.0 / 64
    exact = ml_dtypes.bfloat16
    return np.stack([high, rest], 1), twiddle, pairs.astype(exact), rows.astype(exact)


def dot(left, right):
    return jnp.dot(left, right, preferred_element_type=F32)


def dot_nt(left, right):
    return lax.dot_general(left, right, (((1,), (1,)), ((), ())), preferred_element_type=F32)


def split(values):
    high = values.astype(BF16)
    return high, (values - high.astype(F32)).astype(BF16)


def ordered(index):
    return lax.rem(2 - index + 3 * (index // 2) + 2 * (index // 3) + 4, 4)


def kernel(
    noise_hbm, spec_hbm, order_hbm, tables_hbm, twiddle_hbm, pairs_hbm, rows_hbm,
    modulus_ref, fine_ref, rest_ref,
    order_smem, noise, spec, tables, twiddle, pairs, rows,
    tables_back, s_send, s_recv, n_send, n_recv, mirrored, reversed_, wrapped, scale, f_send, f_recv, b_send, b_recv,
    y_mid, v_high, v_low, v_back, z_high, z_low, w_high, w_low, g_high, g_low,
    r_send, r_recv, r_other, r_send_rest, r_recv_rest, r_other_rest, t_send, t_recv, t_send_rest, t_recv_rest,
    load_sems, send_sems, recv_sems, route_send_sems, route_recv_sems,
):
    zh, y, x, zl, c = [lax.axis_index(a) for a in (*PX, *PY)]
    z = zh * 2 + zl
    line = zh * 64 + y * 16
    column = x * 4 + zl * 2 + c
    me = line + column

    loads = []
    for k, (source, target) in enumerate((
        (spec_hbm, spec), (tables_hbm.at[T_Z], tables.at[T_Z]), (noise_hbm, noise),
        (tables_hbm.at[pl.ds(1, TABLES - 1)], tables.at[pl.ds(1, TABLES - 1)]),
        (twiddle_hbm, twiddle), (pairs_hbm, pairs), (rows_hbm, rows), (order_hbm, order_smem),
    )):
        loads.append(pltpu.make_async_copy(source, target, load_sems.at[k]))
    for load in loads[:3]:
        load.start()

    spots = [(lax.rem(y + dy, 4) * 16 + lax.rem(x + dx, 4) * 4) for dy in (2, 1, 3, 0) for dx in (2, 1, 3, 0)]

    def over_half(action, half):
        core = lax.rem(c + 1 - half, 2)

        def group(s, skip):
            z2 = lax.rem(z + ordered(s), 4)
            base = (z2 // 2) * 64 + lax.rem(z2, 2) * 2 + core
            for k, spot in enumerate(spots):
                if not (skip and k == 15):
                    action(base + spot)

        @pl.loop(0, 4 - half)
        def _(s):
            group(s, False)

        if half:
            group(jnp.int32(3), True)

    def over_devices(action):
        over_half(action, 0)
        over_half(action, 1)

    barrier = pltpu.get_barrier_semaphore()
    over_devices(lambda d: pl.semaphore_signal(barrier, 1, device_id=d, device_id_type=LOGICAL))

    for load in loads[3:]:
        load.start()

    def send(source, target, send_sem, recv_sem):
        return lambda d: pltpu.make_async_remote_copy(
            source(d), target, send_sem, recv_sem, device_id=d, device_id_type=LOGICAL).start()

    def finish(ref, sem):
        pltpu.make_async_copy(ref, ref, sem).wait()

    loads[0].wait()
    for jj in range(4):
        j2lo, m2lo = divmod(jj, 2)
        starts = [(j2lo * 8 + j1) * CY + m2lo * 16 for j1 in range(8)]
        block = jnp.concatenate([spec[pl.ds(s, 16), 0:128] for s in starts], 0)
        s_send[:, jj, :] = block.T
        block = jnp.concatenate([spec[pl.ds(s, 16), 128:256] for s in starts], 0)
        n_send[0, jj, :] = block.T[0]

    row = zh * 4 + y
    on_line = jnp.logical_and(
        lax.broadcasted_iota(jnp.int32, (4, 128), 0) < 2, lax.broadcasted_iota(jnp.int32, (4, 128), 1) < 16)
    low_inside, low_line = jnp.where(row >= 4, 0, 1), jnp.where(column >= 8, 0, 1)
    low_half = jnp.where(jnp.logical_and(on_line, lax.rem(row, 4) == 0), low_line, low_inside) == 1
    lowest, highest = s_send[0], n_send[0]
    s_send[0] = jnp.where(low_half, lowest, highest)
    n_send[0] = jnp.where(low_half, highest, lowest)

    loads[1].wait()
    loads[2].wait()

    @pl.loop(0, 2)
    def _(f):
        for part in range(2):
            high, low = split(noise[f, pl.ds(part * 256, 256), :])
            out = dot_nt(tables[T_Z, 0], high) + dot_nt(tables[T_Z, 0], low) + dot_nt(tables[T_Z, 1], high)
            for ri in range(2):
                for l in range(2):
                    f_send[f, pl.ds(ri * 4 + part * 2 + l, 128, stride=8), :] = (
                        out[ri * 128:(ri + 1) * 128, l * 128:(l + 1) * 128])

    def swap_first(ref):
        first, second = ref[0, pl.ds(0, 8), :], ref[1, pl.ds(0, 8), :]
        ref[0, pl.ds(0, 8), :] = jnp.concatenate([first[:4], second[:4]], 0)
        ref[1, pl.ds(0, 8), :] = jnp.concatenate([first[4:], second[4:]], 0)

    def block_of(d):
        return pl.ds(pl.multiple_of(d * 8, 8), 8)

    swap_first(f_send)
    pl.semaphore_wait(barrier, 127)
    over_devices(send(lambda d: s_send.at[d], s_recv.at[me], send_sems.at[0], recv_sems.at[0]))
    s_recv[me] = s_send[me]
    extra = jnp.logical_and(jnp.logical_and(lax.rem(row, 4) == 0, lax.rem(column, 8) == 0), me != 0)

    @pl.when(extra)
    def _():
        pltpu.make_async_remote_copy(
            n_send.at[0], n_recv.at[(row // 4) * 2 + column // 8], send_sems.at[1], recv_sems.at[1],
            device_id=jnp.int32(0), device_id_type=LOGICAL).start()

    def send_forward(f, half):
        over_half(send(
            lambda d: f_send.at[f, block_of(d)], f_recv.at[f, block_of(me)],
            send_sems.at[2 + 2 * f + half], recv_sems.at[2 + f]), half)

    def forward_sent(f, half):
        finish(f_send.at[f, pl.ds(0, (64 - half) * 8)], send_sems.at[2 + 2 * f + half])

    send_forward(0, 0)
    send_forward(0, 1)
    for f in range(2):
        f_recv[f, block_of(me), :] = f_send[f, block_of(me), :]

    finish(s_recv.at[pl.ds(0, 127)], recv_sems.at[0])

    def arrange(plane, load):
        for j2a in range(4):
            parts = [load(2 * p_high + j2a // 2, (j2a % 2) * 2 + m2lo) for m2lo in range(2) for p_high in range(4)]
            scale[plane, j2a] = jnp.concatenate(parts, 0).T

    def received(p, jj):
        return s_recv[pl.ds(p * 16, 16), jj, :]

    @pl.when(me != 0)
    def _():
        arrange(0, received)

    @pl.when(me == 0)
    def _():
        n_recv[0] = n_send[0]
        finish(n_recv.at[pl.ds(0, 3)], recv_sems.at[1])
        lanes = lax.broadcasted_iota(jnp.int32, (128, 128), 1)
        opposite = lax.rem(8 - lax.div(lanes, 16), 8) * 16 + lax.rem(16 - lax.rem(lanes, 16), 16)
        chosen = jnp.where(lax.broadcasted_iota(jnp.int32, (128, 128), 0) == opposite, 1.0, 0.0).astype(BF16)
        for jj in range(4):
            high, low = split(s_recv[:, jj, :])
            mirrored[:, jj, :] = dot(high, chosen) + dot(low, chosen)

        @pl.loop(0, 8)
        def _(p):
            for q in range(16):
                block = mirrored[p * 16 + q]
                reversed_[p * 16 + 15 - q] = block
                wrapped[p * 16 + (16 - q) % 16] = block

        lane = lax.broadcasted_iota(jnp.int32, (16, 128), 1)

        def opposite_block(p, jj):
            j2lo, m2lo = divmod(jj, 2)

            def over_m(p2, j2):
                spots = pl.ds(p2 * 16, 16)
                ends = wrapped[spots, j2 * 2, :] if m2lo == 0 else reversed_[spots, j2 * 2 + 1, :]
                return jnp.where(lax.rem(lane, 16) == 0, ends, reversed_[spots, j2 * 2 + 1 - m2lo, :])

            ends = over_m((8 - p) % 8, 0) if j2lo == 0 else over_m(7 - p, 1)
            return jnp.where(lane < 16, ends, over_m(7 - p, 1 - j2lo))

        own = lax.broadcasted_iota(jnp.int32, (16, 128), 0)

        def plane_of(plane):
            def load(p, jj):
                block = received(p, jj) if (p >= 4) == (plane == 1) else opposite_block(p, jj)
                if p % 4 == 0 and jj < 2:
                    low, high = received(p, jj), opposite_block(p, jj)
                    if plane == 1:
                        low, high = high, low
                    on = jnp.where(own < 8, low, high)
                    if jj == 0:
                        spot = jnp.logical_and(lane == 0, own == 8 * (1 - plane))
                        on = jnp.where(spot, n_recv[(p // 4) * 2 + 1 - plane, pl.ds(0, 1), :], on)
                    block = jnp.where(lane < 16, on, block)
                return block

            return load

        for plane in range(2):
            arrange(plane, plane_of(plane))

    send_forward(1, 0)
    send_forward(1, 1)
    for load in loads[3:]:
        load.wait()
    for j2a in range(4):
        for k in range(2):
            tables_back[j2a, k] = tables[T_C + j2a, k].astype(F32).T.astype(BF16)

    def send_back(f):
        over_devices(send(
            lambda d: b_send.at[f, block_of(d)], b_recv.at[f, block_of(me)],
            send_sems.at[6 + f], recv_sems.at[4 + f]))

    @pl.loop(0, 2)
    def _(f):
        finish(f_recv.at[f, pl.ds(0, 127 * 8)], recv_sems.at[2 + f])
        for part in range(2):
            values = jnp.concatenate([
                jnp.concatenate([
                    f_recv[f, pl.ds(ri * 4 + part * 2 + l, 128, stride=8), :] for l in range(2)], 1)
                for ri in range(2)], 0)
            high, low = split(values)
            y_mid[:, part * 256:(part + 1) * 256] = (
                dot(tables[T_P, 0], high) + dot(tables[T_P, 0], low) + dot(tables[T_P, 1], high))

        @pl.loop(0, 8)
        def _(n):
            at = pl.multiple_of(n * 16, 16)
            real, imag = [], []
            for l in range(4):
                lanes = slice(l * 128, (l + 1) * 128)
                vr, vi = y_mid[pl.ds(at, 16), lanes], y_mid[pl.ds(128 + at, 16), lanes]
                wr, wi = twiddle[0, pl.ds(at, 16), lanes], twiddle[1, pl.ds(at, 16), lanes]
                real.append(vr * wr - vi * wi)
                imag.append(vr * wi + vi * wr)
            r02, r13 = real[0] + real[2], real[1] + real[3]
            i02, i13 = imag[0] + imag[2], imag[1] + imag[3]
            rd, re = real[0] - real[2], real[1] - real[3]
            id_, ie = imag[0] - imag[2], imag[1] - imag[3]
            outs = ((r02 + r13, i02 + i13), (rd + ie, id_ - re), (r02 - r13, i02 - i13), (rd - ie, id_ + re))
            for j2a, pair in enumerate(outs):
                for ri in range(2):
                    high, low = split(pair[ri])
                    v_high[j2a, pl.ds(at, 16), ri * 128:(ri + 1) * 128] = high
                    v_low[j2a, pl.ds(at, 16), ri * 128:(ri + 1) * 128] = low

        for j2a in range(4):
            high, low = v_high[j2a], v_low[j2a]
            spectral = (dot(high, tables[T_C + j2a, 0]) + dot(low, tables[T_C + j2a, 0])
                        + dot(high, tables[T_C + j2a, 1]))
            factor = scale[jnp.where(me == 0, f, 0), j2a]
            high, low = split(spectral * jnp.concatenate([factor, factor], 1))
            v_back[j2a] = (dot(high, tables_back[j2a, 0]) + dot(low, tables_back[j2a, 0])
                           + dot(high, tables_back[j2a, 1]))

        @pl.loop(0, 8)
        def _(n):
            at = pl.multiple_of(n * 16, 16)
            real = [v_back[j2a, pl.ds(at, 16), 0:128] for j2a in range(4)]
            imag = [v_back[j2a, pl.ds(at, 16), 128:256] for j2a in range(4)]
            r02, r13 = real[0] + real[2], real[1] + real[3]
            i02, i13 = imag[0] + imag[2], imag[1] + imag[3]
            rd, re = real[0] - real[2], real[1] - real[3]
            id_, ie = imag[0] - imag[2], imag[1] - imag[3]
            outs = ((r02 + r13, i02 + i13), (rd - ie, id_ + re), (r02 - r13, i02 - i13), (rd + ie, id_ - re))
            for l, (vr, vi) in enumerate(outs):
                lanes = slice(l * 128, (l + 1) * 128)
                wr, wi = twiddle[0, pl.ds(at, 16), lanes], twiddle[1, pl.ds(at, 16), lanes]
                for ri, value in enumerate((vr * wr + vi * wi, vi * wr - vr * wi)):
                    high, low = split(value)
                    z_high[pl.ds(ri * 128 + at, 16), lanes] = high
                    z_low[pl.ds(ri * 128 + at, 16), lanes] = low

        for part in range(2):
            high, low = z_high[:, part * 256:(part + 1) * 256], z_low[:, part * 256:(part + 1) * 256]
            out = dot(tables[T_PI, 0], high) + dot(tables[T_PI, 0], low) + dot(tables[T_PI, 1], high)
            for ri in range(2):
                for l in range(2):
                    half, row = jnp.where(me == 0, ri, f), jnp.where(me == 0, f, ri)
                    b_send[half, pl.ds(row * 4 + part * 2 + l, 128, stride=8), :] = (
                        out[ri * 128:(ri + 1) * 128, l * 128:(l + 1) * 128])

        @pl.when(jnp.logical_and(me == 0, f == 1))
        def _():
            send_back(0)

        @pl.when(jnp.logical_or(me != 0, f == 1))
        def _():
            send_back(f)

    for f in range(2):
        b_recv[f, block_of(me), :] = b_send[f, block_of(me), :]

    def over_column(action):
        for dx in (2, 1, 3, 0):
            for dz in (1, 0):
                for dc in (1, 0):
                    if (dx, dz, dc) != (0, 0, 0):
                        action(lax.rem(x + dx, 4) * 4 + lax.rem(zl + dz, 2) * 2 + lax.rem(c + dc, 2))

    def send_pieces(f, phase, pairs_of_refs):
        over_column(lambda g: [pltpu.make_async_remote_copy(
            source.at[g], target.at[column], route_send_sems.at[phase + k, f], route_recv_sems.at[phase + k, f],
            device_id=line + g, device_id_type=LOGICAL).start()
            for k, (source, target) in enumerate(pairs_of_refs)])
        for source, target in pairs_of_refs:
            target[column] = source[column]

    def await_pieces(f, phase, pairs_of_refs):
        for k, (_, target) in enumerate(pairs_of_refs):
            finish(target.at[pl.ds(0, 15)], route_recv_sems.at[phase + k, f])

    first_refs = [((r_send.at[0], r_recv), (r_send_rest.at[0], r_recv_rest)),
                  ((r_send.at[1], r_other), (r_send_rest.at[1], r_other_rest))]
    second_refs = [((t_send.at[f], t_recv.at[f]), (t_send_rest.at[f], t_recv_rest.at[f])) for f in range(2)]

    fewer = lax.broadcasted_iota(jnp.int32, (32, 128), 1) < 64

    for f in range(2):
        finish(b_recv.at[f, pl.ds(0, 127 * 8)], recv_sems.at[4 + f])
        for l in range(4):
            cells = pl.ds(l * 128, 128)
            for ri in range(2):
                high, low = split(b_recv[f, pl.ds(ri * 4 + l, 128, stride=8), :].T)
                w_high[cells, ri * 128:(ri + 1) * 128] = high
                w_low[cells, ri * 128:(ri + 1) * 128] = low
        for part in range(2):
            cells = pl.ds(part * 256, 256)
            high, low = w_high[cells, :], w_low[cells, :]
            fields = dot(high, tables[T_U, 0]) + dot(low, tables[T_U, 0]) + dot(high, tables[T_U, 1])
            modulus = jnp.exp(0.5 * fields)
            modulus_ref[f, cells, :] = modulus
            high, low = split(modulus)
            high, low = split(dot(high, pairs[...]) + dot(low, pairs[...]))
            g_high[cells, :] = high
            g_low[cells, :] = low
        coarse = dot(rows[...], g_high[...]) + dot(rows[...], g_low[...])
        r_send[f] = coarse[0:128, 0:128].reshape(16, 8, 128)
        r_send_rest[f] = jnp.where(fewer, coarse[128:160, 128:256], coarse[160:192, 128:256]).reshape(16, 2, 128)
        send_pieces(f, 0, first_refs[f])

    for f in range(2):
        await_pieces(f, 0, first_refs[f])
        (_, held), (_, held_rest) = first_refs[f]

        @pl.loop(0, 16)
        def _(g):
            t_send[f, g] = held[order_smem[0, g]]
            second, third = held_rest[order_smem[1, g]], held_rest[order_smem[2, g]]
            t_send_rest[f, g] = jnp.where(fewer[0:2], second, third)

        send_pieces(f, 2, second_refs[f])

    for f in range(2):
        await_pieces(f, 2, second_refs[f])
        fine_ref[f] = t_recv[f]
        rest_ref[f] = t_recv_rest[f]

    finish(s_send.at[pl.ds(0, 127)], send_sems.at[0])

    @pl.when(extra)
    def _():
        finish(n_send.at[0], send_sems.at[1])

    for f in range(2):
        finish(b_send.at[f, pl.ds(0, 127 * 8)], send_sems.at[6 + f])
        for k, (whole, rest) in enumerate(((r_send, r_send_rest), (t_send, t_send_rest))):
            finish(whole.at[f, pl.ds(0, 15)], route_send_sems.at[2 * k, f])
            finish(rest.at[f, pl.ds(0, 15)], route_send_sems.at[2 * k + 1, f])
    for f in range(2):
        for half in range(2):
            forward_sent(f, half)


def finisher(modulus_ref, fine_ref, rest_ref, modulus_hbm, one_hbm, two_hbm, three_hbm, two, three, sems):
    stores = [
        pltpu.make_async_copy(source, target, sems.at[k]) for k, (source, target) in enumerate((
            (modulus_ref, modulus_hbm), (fine_ref, one_hbm), (two, two_hbm), (three, three_hbm)))]
    stores[0].start()
    stores[1].start()
    for f in range(2):
        rest = rest_ref[f]
        two[pl.ds(f * 32, 32), :] = rest.reshape(32, 128)[:, 0:64]
        three[pl.ds(f * 8, 8), :] = rest[0:8, 0, 64:96]
    stores[2].start()
    stores[3].start()
    for store in stores:
        store.wait()


def on_device(white_noise, spectrum, group_table):
    tables, twiddle, pairs, rows = build_tables()
    hbm = pl.BlockSpec(memory_space=pltpu.HBM)
    vmem = pl.BlockSpec(memory_space=pltpu.VMEM)
    modulus_shape = jax.ShapeDtypeStruct((2, CELLS, NZ), F32)
    modulus, fine, rest = pl.pallas_call(
        kernel,
        out_shape=(pltpu.VMEM((2, CELLS, NZ), F32), pltpu.VMEM((2, 16, 8, 128), F32), pltpu.VMEM((2, 16, 2, 128), F32)),
        in_specs=[hbm] * 7,
        out_specs=(vmem, vmem, vmem),
        scratch_shapes=[
            pltpu.SMEM((3, 16), jnp.int32),
            pltpu.VMEM((2, CELLS, NZ), F32),
            pltpu.VMEM((CELLS, NZ), F32),
            pltpu.VMEM((TABLES, 2, 256, 256), BF16),
            pltpu.VMEM((2, 128, CELLS), F32),
            pltpu.VMEM((NZ, 256), BF16),
            pltpu.VMEM((192, CELLS), BF16),
            pltpu.VMEM((4, 2, 256, 256), BF16),
            pltpu.VMEM((128, 4, 128), F32),
            pltpu.VMEM((128, 4, 128), F32),
            pltpu.VMEM((1, 4, 128), F32),
            pltpu.VMEM((4, 4, 128), F32),
            *[pltpu.VMEM((128, 4, 128), F32)] * 3,
            pltpu.VMEM((2, 4, 128, 128), F32),
            pltpu.VMEM((2, 1024, 128), F32),
            pltpu.VMEM((2, 1024, 128), F32),
            pltpu.VMEM((2, 1024, 128), F32),
            pltpu.VMEM((2, 1024, 128), F32),
            pltpu.VMEM((256, CELLS), F32),
            pltpu.VMEM((4, 128, 256), BF16),
            pltpu.VMEM((4, 128, 256), BF16),
            pltpu.VMEM((4, 128, 256), F32),
            pltpu.VMEM((256, CELLS), BF16),
            pltpu.VMEM((256, CELLS), BF16),
            *[pltpu.VMEM((CELLS, 256), BF16)] * 4,
            *[pltpu.VMEM((*count, 16, size, 128), F32) for size in (8, 2) for count in ((2,), (), ())],
            *[pltpu.VMEM((2, 16, size, 128), F32) for size in (8, 8, 2, 2)],
            pltpu.SemaphoreType.DMA((8,)),
            pltpu.SemaphoreType.DMA((8,)),
            pltpu.SemaphoreType.DMA((6,)),
            pltpu.SemaphoreType.DMA((4, 2)),
            pltpu.SemaphoreType.DMA((4, 2)),
        ],
        compiler_params=pltpu.CompilerParams(
            collective_id=0, has_side_effects=True, vmem_limit_bytes=60000000),
        name="moduli",
    )(
        white_noise.reshape(2, CELLS, NZ), spectrum.reshape(CELLS, NZ), group_table,
        jnp.asarray(tables), jnp.asarray(twiddle), jnp.asarray(pairs), jnp.asarray(rows),
    )
    modulus, one, two, three = pl.pallas_call(
        finisher,
        out_shape=(
            modulus_shape,
            jax.ShapeDtypeStruct((2, 16, 8, 128), F32),
            jax.ShapeDtypeStruct((64, 64), F32),
            jax.ShapeDtypeStruct((16, 32), F32),
        ),
        in_specs=[vmem, vmem, vmem],
        out_specs=(hbm, hbm, hbm, hbm),
        scratch_shapes=[pltpu.VMEM((64, 64), F32), pltpu.VMEM((16, 32), F32), pltpu.SemaphoreType.DMA((4,))],
        compiler_params=pltpu.CompilerParams(vmem_limit_bytes=4 << 20),
        name="levels",
    )(modulus, fine, rest)
    return (
        modulus.reshape(2, CX, CY, NZ),
        one.reshape(2, 8, 16, 128),
        two.reshape(2, 4, 8, 64),
        three.reshape(2, 2, 4, 32),
    )


def solution(mesh):
    split_mesh = Mesh(mesh.devices.reshape(2, 4, 4, 2, 2), (*PX, *PY))
    whole = P(None, PX, PY, None)
    return jax.shard_map(
        on_device,
        mesh=split_mesh,
        in_specs=(whole, P(PX, PY, None), P()),
        out_specs=(whole, whole, whole, whole),
        check_vma=False,
    )
```

```python
import functools

import jax
import jax.numpy as jnp
import ml_dtypes
import numpy as np
from jax import lax
from jax.experimental import pallas as pl
from jax.experimental.pallas import tpu as pltpu
from jax.sharding import Mesh
from jax.sharding import PartitionSpec as P

PX = ("px_0", "px_1")
PY = ("py_0", "py_1", "py_2")
F32 = jnp.float32
BF16 = jnp.bfloat16
LOGICAL = pl.DeviceIdType.LOGICAL

NX, NY, NZ = 128, 512, 256
CX, CY = 16, 32
CELLS = CX * CY
T_Z, T_P, T_C, T_PI, T_U, TABLES = 0, 1, 2, 6, 7, 8


def wave(products, length, sign):
    angles = 2.0 * np.pi * (products % length) / length
    return np.cos(angles), sign * np.sin(angles)


def applied_left(real, imag):
    return np.block([[real, -imag], [imag, real]])


def build_tables():
    spots = np.arange(128)
    z = np.arange(NZ)
    p, q = spots // 16, spots % 16
    j1, m1 = spots // 16, spots % 16
    tables = np.zeros((TABLES, 256, 256))
    cos_z, sin_z = wave(spots[:, None] * z[None, :], NZ, -1.0)
    sin_z[0] = (-1.0) ** z
    tables[T_Z] = np.concatenate([cos_z, sin_z], 0)
    weight = np.where(spots == 0, 1.0, 2.0)[:, None] / float(NX * NY * NZ)
    tables[T_U] = np.concatenate([cos_z * weight, sin_z * weight], 0)
    outer = 2 * p[None, :] * j1[:, None] + q[None, :] * m1[:, None]
    tables[T_P] = applied_left(*wave(outer, 16, -1.0))
    tables[T_PI] = applied_left(*wave(outer.T, 16, 1.0))
    low, b = spots // 32, spots % 32
    half, j2b, q2 = spots // 64, (spots // 16) % 4, spots % 16
    m2 = 2 * q2 + half
    for j2a in range(4):
        inner = 2 * low[:, None] * j2a + 8 * low[:, None] * j2b[None, :] + b[:, None] * m2[None, :]
        tables[T_C + j2a] = applied_left(*wave(inner.T, 32, -1.0)).T
    cell_a, cell_b = np.arange(CELLS) // CY, np.arange(CELLS) % CY
    middle = 4 * cell_a[None, :] * j1[:, None] + cell_b[None, :] * m1[:, None]
    twiddle = np.stack(wave(middle, 512, -1.0)).astype(np.float32)
    high = tables.astype(np.float32).astype(ml_dtypes.bfloat16)
    rest = (tables - high.astype(np.float64)).astype(np.float32).astype(ml_dtypes.bfloat16)
    pairs = np.zeros((NZ, 256))
    pairs[z, z // 2] = 0.5
    pairs[z, 128 + z // 4] = 0.25
    pairs[z, 192 + z // 8] = 0.125
    rows = np.zeros((192, CELLS))
    for cell in range(CELLS):
        a, b = divmod(cell, CY)
        rows[(a // 2) * 16 + b // 2, cell] = 0.25
        rows[128 + (a // 4) * 8 + b // 4, cell] = 1.0 / 16
        rows[160 + 2 * ((a // 8) * 4 + b // 8), cell] = 1.0 / 64
    exact = ml_dtypes.bfloat16
    return np.stack([high, rest], 1), twiddle, pairs.astype(exact), rows.astype(exact)


def dot(left, right):
    return jnp.dot(left, right, preferred_element_type=F32)


def dot_nt(left, right):
    return lax.dot_general(left, right, (((1,), (1,)), ((), ())), preferred_element_type=F32)


def split(values):
    high = values.astype(BF16)
    return high, (values - high.astype(F32)).astype(BF16)


def ordered(index):
    return lax.rem(2 - index + 3 * (index // 2) + 2 * (index // 3) + 4, 4)


def kernel(
    noise_hbm, spec_hbm, order_hbm, tables_hbm, twiddle_hbm, pairs_hbm, rows_hbm,
    modulus_ref, fine_ref, rest_ref,
    order_smem, noise, spec, tables, twiddle, pairs, rows,
    tables_back, s_send, s_recv, n_send, n_recv, mirrored, reversed_, wrapped, scale, f_send, f_recv, b_send, b_recv,
    y_mid, v_high, v_low, v_back, z_high, z_low, w_high, w_low, g_high, g_low,
    r_send, r_recv, r_other, r_send_rest, r_recv_rest, r_other_rest, t_send, t_recv, t_send_rest, t_recv_rest,
    load_sems, send_sems, recv_sems, route_send_sems, route_recv_sems,
):
    zh, y, x, zl, c = [lax.axis_index(a) for a in (*PX, *PY)]
    z = zh * 2 + zl
    line = zh * 64 + y * 16
    column = x * 4 + zl * 2 + c
    me = line + column

    loads = []
    for k, (source, target) in enumerate((
        (spec_hbm, spec), (tables_hbm.at[T_Z], tables.at[T_Z]), (noise_hbm, noise),
        (tables_hbm.at[pl.ds(1, TABLES - 1)], tables.at[pl.ds(1, TABLES - 1)]),
        (twiddle_hbm, twiddle), (pairs_hbm, pairs), (rows_hbm, rows), (order_hbm, order_smem),
    )):
        loads.append(pltpu.make_async_copy(source, target, load_sems.at[k]))
    for load in loads[:3]:
        load.start()

    spots = [(lax.rem(y + dy, 4) * 16 + lax.rem(x + dx, 4) * 4) for dy in (2, 1, 3, 0) for dx in (2, 1, 3, 0)]

    def over_half(action, half):
        core = lax.rem(c + 1 - half, 2)

        def group(s, skip):
            z2 = lax.rem(z + ordered(s), 4)
            base = (z2 // 2) * 64 + lax.rem(z2, 2) * 2 + core
            for k, spot in enumerate(spots):
                if not (skip and k == 15):
                    action(base + spot)

        @pl.loop(0, 4 - half)
        def _(s):
            group(s, False)

        if half:
            group(jnp.int32(3), True)

    def over_devices(action):
        over_half(action, 0)
        over_half(action, 1)

    barrier = pltpu.get_barrier_semaphore()
    over_devices(lambda d: pl.semaphore_signal(barrier, 1, device_id=d, device_id_type=LOGICAL))

    for load in loads[3:]:
        load.start()

    def send(source, target, send_sem, recv_sem):
        return lambda d: pltpu.make_async_remote_copy(
            source(d), target, send_sem, recv_sem, device_id=d, device_id_type=LOGICAL).start()

    def finish(ref, sem):
        pltpu.make_async_copy(ref, ref, sem).wait()

    loads[0].wait()
    for jj in range(4):
        j2lo, m2lo = divmod(jj, 2)
        starts = [(j2lo * 8 + j1) * CY + m2lo * 16 for j1 in range(8)]
        block = jnp.concatenate([spec[pl.ds(s, 16), 0:128] for s in starts], 0)
        s_send[:, jj, :] = block.T
        block = jnp.concatenate([spec[pl.ds(s, 16), 128:256] for s in starts], 0)
        n_send[0, jj, :] = block.T[0]

    row = zh * 4 + y
    on_line = jnp.logical_and(
        lax.broadcasted_iota(jnp.int32, (4, 128), 0) < 2, lax.broadcasted_iota(jnp.int32, (4, 128), 1) < 16)
    low_inside, low_line = jnp.where(row >= 4, 0, 1), jnp.where(column >= 8, 0, 1)
    low_half = jnp.where(jnp.logical_and(on_line, lax.rem(row, 4) == 0), low_line, low_inside) == 1
    lowest, highest = s_send[0], n_send[0]
    s_send[0] = jnp.where(low_half, lowest, highest)
    n_send[0] = jnp.where(low_half, highest, lowest)

    loads[1].wait()
    loads[2].wait()

    @pl.loop(0, 2)
    def _(f):
        for part in range(2):
            high, low = split(noise[f, pl.ds(part * 256, 256), :])
            out = dot_nt(tables[T_Z, 0], high) + dot_nt(tables[T_Z, 0], low) + dot_nt(tables[T_Z, 1], high)
            for ri in range(2):
                for l in range(2):
                    f_send[f, pl.ds(ri * 4 + part * 2 + l, 128, stride=8), :] = (
                        out[ri * 128:(ri + 1) * 128, l * 128:(l + 1) * 128])

    def swap_first(ref):
        first, second = ref[0, pl.ds(0, 8), :], ref[1, pl.ds(0, 8), :]
        ref[0, pl.ds(0, 8), :] = jnp.concatenate([first[:4], second[:4]], 0)
        ref[1, pl.ds(0, 8), :] = jnp.concatenate([first[4:], second[4:]], 0)

    def block_of(d):
        return pl.ds(pl.multiple_of(d * 8, 8), 8)

    swap_first(f_send)
    pl.semaphore_wait(barrier, 127)
    over_devices(send(lambda d: s_send.at[d], s_recv.at[me], send_sems.at[0], recv_sems.at[0]))
    s_recv[me] = s_send[me]
    extra = jnp.logical_and(jnp.logical_and(lax.rem(row, 4) == 0, lax.rem(column, 8) == 0), me != 0)

    @pl.when(extra)
    def _():
        pltpu.make_async_remote_copy(
            n_send.at[0], n_recv.at[(row // 4) * 2 + column // 8], send_sems.at[1], recv_sems.at[1],
            device_id=jnp.int32(0), device_id_type=LOGICAL).start()

    def send_forward(f, half):
        over_half(send(
            lambda d: f_send.at[f, block_of(d)], f_recv.at[f, block_of(me)],
            send_sems.at[2 + 2 * f + half], recv_sems.at[2 + f]), half)

    def forward_sent(f, half):
        finish(f_send.at[f, pl.ds(0, (64 - half) * 8)], send_sems.at[2 + 2 * f + half])

    send_forward(0, 0)
    send_forward(0, 1)
    for f in range(2):
        f_recv[f, block_of(me), :] = f_send[f, block_of(me), :]

    finish(s_recv.at[pl.ds(0, 127)], recv_sems.at[0])

    def arrange(plane, load):
        for j2a in range(4):
            parts = [load(2 * p_high + j2a // 2, (j2a % 2) * 2 + m2lo) for m2lo in range(2) for p_high in range(4)]
            scale[plane, j2a] = jnp.concatenate(parts, 0).T

    def received(p, jj):
        return s_recv[pl.ds(p * 16, 16), jj, :]

    @pl.when(me != 0)
    def _():
        arrange(0, received)

    @pl.when(me == 0)
    def _():
        n_recv[0] = n_send[0]
        finish(n_recv.at[pl.ds(0, 3)], recv_sems.at[1])
        lanes = lax.broadcasted_iota(jnp.int32, (128, 128), 1)
        opposite = lax.rem(8 - lax.div(lanes, 16), 8) * 16 + lax.rem(16 - lax.rem(lanes, 16), 16)
        chosen = jnp.where(lax.broadcasted_iota(jnp.int32, (128, 128), 0) == opposite, 1.0, 0.0).astype(BF16)
        for jj in range(4):
            high, low = split(s_recv[:, jj, :])
            mirrored[:, jj, :] = dot(high, chosen) + dot(low, chosen)

        @pl.loop(0, 8)
        def _(p):
            for q in range(16):
                block = mirrored[p * 16 + q]
                reversed_[p * 16 + 15 - q] = block
                wrapped[p * 16 + (16 - q) % 16] = block

        lane = lax.broadcasted_iota(jnp.int32, (16, 128), 1)

        def opposite_block(p, jj):
            j2lo, m2lo = divmod(jj, 2)

            def over_m(p2, j2):
                spots = pl.ds(p2 * 16, 16)
                ends = wrapped[spots, j2 * 2, :] if m2lo == 0 else reversed_[spots, j2 * 2 + 1, :]
                return jnp.where(lax.rem(lane, 16) == 0, ends, reversed_[spots, j2 * 2 + 1 - m2lo, :])

            ends = over_m((8 - p) % 8, 0) if j2lo == 0 else over_m(7 - p, 1)
            return jnp.where(lane < 16, ends, over_m(7 - p, 1 - j2lo))

        own = lax.broadcasted_iota(jnp.int32, (16, 128), 0)

        def plane_of(plane):
            def load(p, jj):
                block = received(p, jj) if (p >= 4) == (plane == 1) else opposite_block(p, jj)
                if p % 4 == 0 and jj < 2:
                    low, high = received(p, jj), opposite_block(p, jj)
                    if plane == 1:
                        low, high = high, low
                    on = jnp.where(own < 8, low, high)
                    if jj == 0:
                        spot = jnp.logical_and(lane == 0, own == 8 * (1 - plane))
                        on = jnp.where(spot, n_recv[(p // 4) * 2 + 1 - plane, pl.ds(0, 1), :], on)
                    block = jnp.where(lane < 16, on, block)
                return block

            return load

        for plane in range(2):
            arrange(plane, plane_of(plane))

    send_forward(1, 0)
    send_forward(1, 1)
    for load in loads[3:]:
        load.wait()
    for j2a in range(4):
        for k in range(2):
            tables_back[j2a, k] = tables[T_C + j2a, k].astype(F32).T.astype(BF16)

    def send_back(f):
        for half in (1, 0):
            over_half(send(
                lambda d: b_send.at[f, block_of(d)], b_recv.at[f, block_of(me)],
                send_sems.at[6 + f], recv_sems.at[4 + f]), half)

    @pl.loop(0, 2)
    def _(f):
        finish(f_recv.at[f, pl.ds(0, 127 * 8)], recv_sems.at[2 + f])
        for part in range(2):
            values = jnp.concatenate([
                jnp.concatenate([
                    f_recv[f, pl.ds(ri * 4 + part * 2 + l, 128, stride=8), :] for l in range(2)], 1)
                for ri in range(2)], 0)
            high, low = split(values)
            y_mid[:, part * 256:(part + 1) * 256] = (
                dot(tables[T_P, 0], high) + dot(tables[T_P, 0], low) + dot(tables[T_P, 1], high))

        @pl.loop(0, 8)
        def _(n):
            at = pl.multiple_of(n * 16, 16)
            real, imag = [], []
            for l in range(4):
                lanes = slice(l * 128, (l + 1) * 128)
                vr, vi = y_mid[pl.ds(at, 16), lanes], y_mid[pl.ds(128 + at, 16), lanes]
                wr, wi = twiddle[0, pl.ds(at, 16), lanes], twiddle[1, pl.ds(at, 16), lanes]
                real.append(vr * wr - vi * wi)
                imag.append(vr * wi + vi * wr)
            r02, r13 = real[0] + real[2], real[1] + real[3]
            i02, i13 = imag[0] + imag[2], imag[1] + imag[3]
            rd, re = real[0] - real[2], real[1] - real[3]
            id_, ie = imag[0] - imag[2], imag[1] - imag[3]
            outs = ((r02 + r13, i02 + i13), (rd + ie, id_ - re), (r02 - r13, i02 - i13), (rd - ie, id_ + re))
            for j2a, pair in enumerate(outs):
                for ri in range(2):
                    high, low = split(pair[ri])
                    v_high[j2a, pl.ds(at, 16), ri * 128:(ri + 1) * 128] = high
                    v_low[j2a, pl.ds(at, 16), ri * 128:(ri + 1) * 128] = low

        for j2a in range(4):
            high, low = v_high[j2a], v_low[j2a]
            spectral = (dot(high, tables[T_C + j2a, 0]) + dot(low, tables[T_C + j2a, 0])
                        + dot(high, tables[T_C + j2a, 1]))
            factor = scale[jnp.where(me == 0, f, 0), j2a]
            high, low = split(spectral * jnp.concatenate([factor, factor], 1))
            v_back[j2a] = (dot(high, tables_back[j2a, 0]) + dot(low, tables_back[j2a, 0])
                           + dot(high, tables_back[j2a, 1]))

        @pl.loop(0, 8)
        def _(n):
            at = pl.multiple_of(n * 16, 16)
            real = [v_back[j2a, pl.ds(at, 16), 0:128] for j2a in range(4)]
            imag = [v_back[j2a, pl.ds(at, 16), 128:256] for j2a in range(4)]
            r02, r13 = real[0] + real[2], real[1] + real[3]
            i02, i13 = imag[0] + imag[2], imag[1] + imag[3]
            rd, re = real[0] - real[2], real[1] - real[3]
            id_, ie = imag[0] - imag[2], imag[1] - imag[3]
            outs = ((r02 + r13, i02 + i13), (rd - ie, id_ + re), (r02 - r13, i02 - i13), (rd + ie, id_ - re))
            for l, (vr, vi) in enumerate(outs):
                lanes = slice(l * 128, (l + 1) * 128)
                wr, wi = twiddle[0, pl.ds(at, 16), lanes], twiddle[1, pl.ds(at, 16), lanes]
                for ri, value in enumerate((vr * wr + vi * wi, vi * wr - vr * wi)):
                    high, low = split(value)
                    z_high[pl.ds(ri * 128 + at, 16), lanes] = high
                    z_low[pl.ds(ri * 128 + at, 16), lanes] = low

        for part in range(2):
            high, low = z_high[:, part * 256:(part + 1) * 256], z_low[:, part * 256:(part + 1) * 256]
            out = dot(tables[T_PI, 0], high) + dot(tables[T_PI, 0], low) + dot(tables[T_PI, 1], high)
            for ri in range(2):
                for l in range(2):
                    half, row = jnp.where(me == 0, ri, f), jnp.where(me == 0, f, ri)
                    b_send[half, pl.ds(row * 4 + part * 2 + l, 128, stride=8), :] = (
                        out[ri * 128:(ri + 1) * 128, l * 128:(l + 1) * 128])

        @pl.when(jnp.logical_and(me == 0, f == 1))
        def _():
            send_back(0)

        @pl.when(jnp.logical_or(me != 0, f == 1))
        def _():
            send_back(f)

    for f in range(2):
        b_recv[f, block_of(me), :] = b_send[f, block_of(me), :]

    def over_column(action):
        for dx in (2, 1, 3, 0):
            for dz in (1, 0):
                for dc in (1, 0):
                    if (dx, dz, dc) != (0, 0, 0):
                        action(lax.rem(x + dx, 4) * 4 + lax.rem(zl + dz, 2) * 2 + lax.rem(c + dc, 2))

    def send_pieces(f, phase, pairs_of_refs):
        over_column(lambda g: [pltpu.make_async_remote_copy(
            source.at[g], target.at[column], route_send_sems.at[phase + k, f], route_recv_sems.at[phase + k, f],
            device_id=line + g, device_id_type=LOGICAL).start()
            for k, (source, target) in enumerate(pairs_of_refs)])
        for source, target in pairs_of_refs:
            target[column] = source[column]

    def await_pieces(f, phase, pairs_of_refs):
        for k, (_, target) in enumerate(pairs_of_refs):
            finish(target.at[pl.ds(0, 15)], route_recv_sems.at[phase + k, f])

    first_refs = [((r_send.at[0], r_recv), (r_send_rest.at[0], r_recv_rest)),
                  ((r_send.at[1], r_other), (r_send_rest.at[1], r_other_rest))]
    second_refs = [((t_send.at[f], t_recv.at[f]), (t_send_rest.at[f], t_recv_rest.at[f])) for f in range(2)]

    fewer = lax.broadcasted_iota(jnp.int32, (32, 128), 1) < 64

    for f in range(2):
        finish(b_recv.at[f, pl.ds(0, 127 * 8)], recv_sems.at[4 + f])
        for l in range(4):
            cells = pl.ds(l * 128, 128)
            for ri in range(2):
                high, low = split(b_recv[f, pl.ds(ri * 4 + l, 128, stride=8), :].T)
                w_high[cells, ri * 128:(ri + 1) * 128] = high
                w_low[cells, ri * 128:(ri + 1) * 128] = low
        for part in range(2):
            cells = pl.ds(part * 256, 256)
            high, low = w_high[cells, :], w_low[cells, :]
            fields = dot(high, tables[T_U, 0]) + dot(low, tables[T_U, 0]) + dot(high, tables[T_U, 1])
            modulus = jnp.exp(0.5 * fields)
            modulus_ref[f, cells, :] = modulus
            high, low = split(modulus)
            high, low = split(dot(high, pairs[...]) + dot(low, pairs[...]))
            g_high[cells, :] = high
            g_low[cells, :] = low
        coarse = dot(rows[...], g_high[...]) + dot(rows[...], g_low[...])
        r_send[f] = coarse[0:128, 0:128].reshape(16, 8, 128)
        r_send_rest[f] = jnp.where(fewer, coarse[128:160, 128:256], coarse[160:192, 128:256]).reshape(16, 2, 128)
        send_pieces(f, 0, first_refs[f])

    for f in range(2):
        await_pieces(f, 0, first_refs[f])
        (_, held), (_, held_rest) = first_refs[f]

        @pl.loop(0, 16)
        def _(g):
            t_send[f, g] = held[order_smem[0, g]]
            second, third = held_rest[order_smem[1, g]], held_rest[order_smem[2, g]]
            t_send_rest[f, g] = jnp.where(fewer[0:2], second, third)

        send_pieces(f, 2, second_refs[f])

    for f in range(2):
        await_pieces(f, 2, second_refs[f])
        fine_ref[f] = t_recv[f]
        rest_ref[f] = t_recv_rest[f]

    finish(s_send.at[pl.ds(0, 127)], send_sems.at[0])

    @pl.when(extra)
    def _():
        finish(n_send.at[0], send_sems.at[1])

    for f in range(2):
        finish(b_send.at[f, pl.ds(0, 127 * 8)], send_sems.at[6 + f])
        for k, (whole, rest) in enumerate(((r_send, r_send_rest), (t_send, t_send_rest))):
            finish(whole.at[f, pl.ds(0, 15)], route_send_sems.at[2 * k, f])
            finish(rest.at[f, pl.ds(0, 15)], route_send_sems.at[2 * k + 1, f])
    for f in range(2):
        for half in range(2):
            forward_sent(f, half)


def finisher(modulus_ref, fine_ref, rest_ref, modulus_hbm, one_hbm, two_hbm, three_hbm, two, three, sems):
    stores = [
        pltpu.make_async_copy(source, target, sems.at[k]) for k, (source, target) in enumerate((
            (modulus_ref, modulus_hbm), (fine_ref, one_hbm), (two, two_hbm), (three, three_hbm)))]
    stores[0].start()
    stores[1].start()
    for f in range(2):
        rest = rest_ref[f]
        two[pl.ds(f * 32, 32), :] = rest.reshape(32, 128)[:, 0:64]
        three[pl.ds(f * 8, 8), :] = rest[0:8, 0, 64:96]
    stores[2].start()
    stores[3].start()
    for store in stores:
        store.wait()


def on_device(white_noise, spectrum, group_table):
    tables, twiddle, pairs, rows = build_tables()
    hbm = pl.BlockSpec(memory_space=pltpu.HBM)
    vmem = pl.BlockSpec(memory_space=pltpu.VMEM)
    modulus_shape = jax.ShapeDtypeStruct((2, CELLS, NZ), F32)
    modulus, fine, rest = pl.pallas_call(
        kernel,
        out_shape=(pltpu.VMEM((2, CELLS, NZ), F32), pltpu.VMEM((2, 16, 8, 128), F32), pltpu.VMEM((2, 16, 2, 128), F32)),
        in_specs=[hbm] * 7,
        out_specs=(vmem, vmem, vmem),
        scratch_shapes=[
            pltpu.SMEM((3, 16), jnp.int32),
            pltpu.VMEM((2, CELLS, NZ), F32),
            pltpu.VMEM((CELLS, NZ), F32),
            pltpu.VMEM((TABLES, 2, 256, 256), BF16),
            pltpu.VMEM((2, 128, CELLS), F32),
            pltpu.VMEM((NZ, 256), BF16),
            pltpu.VMEM((192, CELLS), BF16),
            pltpu.VMEM((4, 2, 256, 256), BF16),
            pltpu.VMEM((128, 4, 128), F32),
            pltpu.VMEM((128, 4, 128), F32),
            pltpu.VMEM((1, 4, 128), F32),
            pltpu.VMEM((4, 4, 128), F32),
            *[pltpu.VMEM((128, 4, 128), F32)] * 3,
            pltpu.VMEM((2, 4, 128, 128), F32),
            pltpu.VMEM((2, 1024, 128), F32),
            pltpu.VMEM((2, 1024, 128), F32),
            pltpu.VMEM((2, 1024, 128), F32),
            pltpu.VMEM((2, 1024, 128), F32),
            pltpu.VMEM((256, CELLS), F32),
            pltpu.VMEM((4, 128, 256), BF16),
            pltpu.VMEM((4, 128, 256), BF16),
            pltpu.VMEM((4, 128, 256), F32),
            pltpu.VMEM((256, CELLS), BF16),
            pltpu.VMEM((256, CELLS), BF16),
            *[pltpu.VMEM((CELLS, 256), BF16)] * 4,
            *[pltpu.VMEM((*count, 16, size, 128), F32) for size in (8, 2) for count in ((2,), (), ())],
            *[pltpu.VMEM((2, 16, size, 128), F32) for size in (8, 8, 2, 2)],
            pltpu.SemaphoreType.DMA((8,)),
            pltpu.SemaphoreType.DMA((8,)),
            pltpu.SemaphoreType.DMA((6,)),
            pltpu.SemaphoreType.DMA((4, 2)),
            pltpu.SemaphoreType.DMA((4, 2)),
        ],
        compiler_params=pltpu.CompilerParams(
            collective_id=0, has_side_effects=True, vmem_limit_bytes=60000000),
        name="moduli",
    )(
        white_noise.reshape(2, CELLS, NZ), spectrum.reshape(CELLS, NZ), group_table,
        jnp.asarray(tables), jnp.asarray(twiddle), jnp.asarray(pairs), jnp.asarray(rows),
    )
    modulus, one, two, three = pl.pallas_call(
        finisher,
        out_shape=(
            modulus_shape,
            jax.ShapeDtypeStruct((2, 16, 8, 128), F32),
            jax.ShapeDtypeStruct((64, 64), F32),
            jax.ShapeDtypeStruct((16, 32), F32),
        ),
        in_specs=[vmem, vmem, vmem],
        out_specs=(hbm, hbm, hbm, hbm),
        scratch_shapes=[pltpu.VMEM((64, 64), F32), pltpu.VMEM((16, 32), F32), pltpu.SemaphoreType.DMA((4,))],
        compiler_params=pltpu.CompilerParams(vmem_limit_bytes=4 << 20),
        name="levels",
    )(modulus, fine, rest)
    return (
        modulus.reshape(2, CX, CY, NZ),
        one.reshape(2, 8, 16, 128),
        two.reshape(2, 4, 8, 64),
        three.reshape(2, 2, 4, 32),
    )


def solution(mesh):
    split_mesh = Mesh(mesh.devices.reshape(2, 4, 4, 2, 2), (*PX, *PY))
    whole = P(None, PX, PY, None)
    return jax.shard_map(
        on_device,
        mesh=split_mesh,
        in_specs=(whole, P(PX, PY, None), P()),
        out_specs=(whole, whole, whole, whole),
        check_vma=False,
    )
```

```python
import functools

import jax
import jax.numpy as jnp
import ml_dtypes
import numpy as np
from jax import lax
from jax.experimental import pallas as pl
from jax.experimental.pallas import tpu as pltpu
from jax.sharding import Mesh
from jax.sharding import PartitionSpec as P

PX = ("px_0", "px_1")
PY = ("py_0", "py_1", "py_2")
F32 = jnp.float32
BF16 = jnp.bfloat16
LOGICAL = pl.DeviceIdType.LOGICAL

NX, NY, NZ = 128, 512, 256
CX, CY = 16, 32
CELLS = CX * CY
T_Z, T_P, T_C, T_PI, T_U, TABLES = 0, 1, 2, 6, 7, 8


def wave(products, length, sign):
    angles = 2.0 * np.pi * (products % length) / length
    return np.cos(angles), sign * np.sin(angles)


def applied_left(real, imag):
    return np.block([[real, -imag], [imag, real]])


def build_tables():
    spots = np.arange(128)
    z = np.arange(NZ)
    p, q = spots // 16, spots % 16
    j1, m1 = spots // 16, spots % 16
    tables = np.zeros((TABLES, 256, 256))
    cos_z, sin_z = wave(spots[:, None] * z[None, :], NZ, -1.0)
    sin_z[0] = (-1.0) ** z
    tables[T_Z] = np.concatenate([cos_z, sin_z], 0)
    weight = np.where(spots == 0, 1.0, 2.0)[:, None] / float(NX * NY * NZ)
    tables[T_U] = np.concatenate([cos_z * weight, sin_z * weight], 0)
    outer = 2 * p[None, :] * j1[:, None] + q[None, :] * m1[:, None]
    tables[T_P] = applied_left(*wave(outer, 16, -1.0))
    tables[T_PI] = applied_left(*wave(outer.T, 16, 1.0))
    low, b = spots // 32, spots % 32
    half, j2b, q2 = spots // 64, (spots // 16) % 4, spots % 16
    m2 = 2 * q2 + half
    for j2a in range(4):
        inner = 2 * low[:, None] * j2a + 8 * low[:, None] * j2b[None, :] + b[:, None] * m2[None, :]
        tables[T_C + j2a] = applied_left(*wave(inner.T, 32, -1.0)).T
    cell_a, cell_b = np.arange(CELLS) // CY, np.arange(CELLS) % CY
    middle = 4 * cell_a[None, :] * j1[:, None] + cell_b[None, :] * m1[:, None]
    twiddle = np.stack(wave(middle, 512, -1.0)).astype(np.float32)
    high = tables.astype(np.float32).astype(ml_dtypes.bfloat16)
    rest = (tables - high.astype(np.float64)).astype(np.float32).astype(ml_dtypes.bfloat16)
    pairs = np.zeros((NZ, 256))
    pairs[z, z // 2] = 0.5
    pairs[z, 128 + z // 4] = 0.25
    pairs[z, 192 + z // 8] = 0.125
    rows = np.zeros((192, CELLS))
    for cell in range(CELLS):
        a, b = divmod(cell, CY)
        rows[(a // 2) * 16 + b // 2, cell] = 0.25
        rows[128 + (a // 4) * 8 + b // 4, cell] = 1.0 / 16
        rows[160 + 2 * ((a // 8) * 4 + b // 8), cell] = 1.0 / 64
    exact = ml_dtypes.bfloat16
    return np.stack([high, rest], 1), twiddle, pairs.astype(exact), rows.astype(exact)


def dot(left, right):
    return jnp.dot(left, right, preferred_element_type=F32)


def dot_nt(left, right):
    return lax.dot_general(left, right, (((1,), (1,)), ((), ())), preferred_element_type=F32)


def split(values):
    high = values.astype(BF16)
    return high, (values - high.astype(F32)).astype(BF16)


def ordered(index):
    return lax.rem(2 - index + 3 * (index // 2) + 2 * (index // 3) + 4, 4)


def kernel(
    noise_hbm, spec_hbm, order_hbm, tables_hbm, twiddle_hbm, pairs_hbm, rows_hbm,
    modulus_ref, fine_ref, rest_ref,
    order_smem, noise, spec, tables, twiddle, pairs, rows,
    tables_back, s_send, s_recv, n_send, n_recv, mirrored, reversed_, wrapped, scale, f_send, f_recv, b_send, b_recv,
    y_mid, v_high, v_low, v_back, z_high, z_low, w_high, w_low, g_high, g_low,
    r_send, r_recv, r_other, r_send_rest, r_recv_rest, r_other_rest, t_send, t_recv, t_send_rest, t_recv_rest,
    load_sems, send_sems, recv_sems, route_send_sems, route_recv_sems,
):
    zh, y, x, zl, c = [lax.axis_index(a) for a in (*PX, *PY)]
    z = zh * 2 + zl
    line = zh * 64 + y * 16
    column = x * 4 + zl * 2 + c
    me = line + column

    loads = []
    for k, (source, target) in enumerate((
        (spec_hbm, spec), (tables_hbm.at[T_Z], tables.at[T_Z]), (noise_hbm, noise),
        (tables_hbm.at[pl.ds(1, TABLES - 1)], tables.at[pl.ds(1, TABLES - 1)]),
        (twiddle_hbm, twiddle), (pairs_hbm, pairs), (rows_hbm, rows), (order_hbm, order_smem),
    )):
        loads.append(pltpu.make_async_copy(source, target, load_sems.at[k]))
    for load in loads[:3]:
        load.start()

    spots = [(lax.rem(y + dy, 4) * 16 + lax.rem(x + dx, 4) * 4) for dy in (2, 1, 3, 0) for dx in (2, 1, 3, 0)]

    def over_half(action, half):
        core = lax.rem(c + 1 - half, 2)

        def group(s, skip):
            z2 = lax.rem(z + ordered(s), 4)
            base = (z2 // 2) * 64 + lax.rem(z2, 2) * 2 + core
            for k, spot in enumerate(spots):
                if not (skip and k == 15):
                    action(base + spot)

        @pl.loop(0, 4 - half)
        def _(s):
            group(s, False)

        if half:
            group(jnp.int32(3), True)

    def over_devices(action):
        over_half(action, 0)
        over_half(action, 1)

    barrier = pltpu.get_barrier_semaphore()
    over_devices(lambda d: pl.semaphore_signal(barrier, 1, device_id=d, device_id_type=LOGICAL))

    for load in loads[3:]:
        load.start()

    def send(source, target, send_sem, recv_sem):
        return lambda d: pltpu.make_async_remote_copy(
            source(d), target, send_sem, recv_sem, device_id=d, device_id_type=LOGICAL).start()

    def finish(ref, sem):
        pltpu.make_async_copy(ref, ref, sem).wait()

    loads[0].wait()
    for jj in range(4):
        j2lo, m2lo = divmod(jj, 2)
        starts = [(j2lo * 8 + j1) * CY + m2lo * 16 for j1 in range(8)]
        block = jnp.concatenate([spec[pl.ds(s, 16), 0:128] for s in starts], 0)
        s_send[:, jj, :] = block.T
        block = jnp.concatenate([spec[pl.ds(s, 16), 128:256] for s in starts], 0)
        n_send[0, jj, :] = block.T[0]

    row = zh * 4 + y
    on_line = jnp.logical_and(
        lax.broadcasted_iota(jnp.int32, (4, 128), 0) < 2, lax.broadcasted_iota(jnp.int32, (4, 128), 1) < 16)
    low_inside, low_line = jnp.where(row >= 4, 0, 1), jnp.where(column >= 8, 0, 1)
    low_half = jnp.where(jnp.logical_and(on_line, lax.rem(row, 4) == 0), low_line, low_inside) == 1
    lowest, highest = s_send[0], n_send[0]
    s_send[0] = jnp.where(low_half, lowest, highest)
    n_send[0] = jnp.where(low_half, highest, lowest)

    loads[1].wait()
    loads[2].wait()

    @pl.loop(0, 2)
    def _(f):
        for part in range(2):
            high, low = split(noise[f, pl.ds(part * 256, 256), :])
            out = dot_nt(tables[T_Z, 0], high) + dot_nt(tables[T_Z, 0], low) + dot_nt(tables[T_Z, 1], high)
            for ri in range(2):
                for l in range(2):
                    f_send[f, pl.ds(ri * 4 + part * 2 + l, 128, stride=8), :] = (
                        out[ri * 128:(ri + 1) * 128, l * 128:(l + 1) * 128])

    def swap_first(ref):
        first, second = ref[0, pl.ds(0, 8), :], ref[1, pl.ds(0, 8), :]
        ref[0, pl.ds(0, 8), :] = jnp.concatenate([first[:4], second[:4]], 0)
        ref[1, pl.ds(0, 8), :] = jnp.concatenate([first[4:], second[4:]], 0)

    def block_of(d):
        return pl.ds(pl.multiple_of(d * 8, 8), 8)

    swap_first(f_send)
    pl.semaphore_wait(barrier, 127)
    for half in (1, 0):
        over_half(send(lambda d: s_send.at[d], s_recv.at[me], send_sems.at[0], recv_sems.at[0]), half)
    s_recv[me] = s_send[me]
    extra = jnp.logical_and(jnp.logical_and(lax.rem(row, 4) == 0, lax.rem(column, 8) == 0), me != 0)

    @pl.when(extra)
    def _():
        pltpu.make_async_remote_copy(
            n_send.at[0], n_recv.at[(row // 4) * 2 + column // 8], send_sems.at[1], recv_sems.at[1],
            device_id=jnp.int32(0), device_id_type=LOGICAL).start()

    def send_forward(f, half):
        over_half(send(
            lambda d: f_send.at[f, block_of(d)], f_recv.at[f, block_of(me)],
            send_sems.at[2 + 2 * f + half], recv_sems.at[2 + f]), half)

    def forward_sent(f, half):
        finish(f_send.at[f, pl.ds(0, (64 - half) * 8)], send_sems.at[2 + 2 * f + half])

    send_forward(0, 1)
    send_forward(0, 0)
    for f in range(2):
        f_recv[f, block_of(me), :] = f_send[f, block_of(me), :]

    finish(s_recv.at[pl.ds(0, 127)], recv_sems.at[0])

    def arrange(plane, load):
        for j2a in range(4):
            parts = [load(2 * p_high + j2a // 2, (j2a % 2) * 2 + m2lo) for m2lo in range(2) for p_high in range(4)]
            scale[plane, j2a] = jnp.concatenate(parts, 0).T

    def received(p, jj):
        return s_recv[pl.ds(p * 16, 16), jj, :]

    @pl.when(me != 0)
    def _():
        arrange(0, received)

    @pl.when(me == 0)
    def _():
        n_recv[0] = n_send[0]
        finish(n_recv.at[pl.ds(0, 3)], recv_sems.at[1])
        lanes = lax.broadcasted_iota(jnp.int32, (128, 128), 1)
        opposite = lax.rem(8 - lax.div(lanes, 16), 8) * 16 + lax.rem(16 - lax.rem(lanes, 16), 16)
        chosen = jnp.where(lax.broadcasted_iota(jnp.int32, (128, 128), 0) == opposite, 1.0, 0.0).astype(BF16)
        for jj in range(4):
            high, low = split(s_recv[:, jj, :])
            mirrored[:, jj, :] = dot(high, chosen) + dot(low, chosen)

        @pl.loop(0, 8)
        def _(p):
            for q in range(16):
                block = mirrored[p * 16 + q]
                reversed_[p * 16 + 15 - q] = block
                wrapped[p * 16 + (16 - q) % 16] = block

        lane = lax.broadcasted_iota(jnp.int32, (16, 128), 1)

        def opposite_block(p, jj):
            j2lo, m2lo = divmod(jj, 2)

            def over_m(p2, j2):
                spots = pl.ds(p2 * 16, 16)
                ends = wrapped[spots, j2 * 2, :] if m2lo == 0 else reversed_[spots, j2 * 2 + 1, :]
                return jnp.where(lax.rem(lane, 16) == 0, ends, reversed_[spots, j2 * 2 + 1 - m2lo, :])

            ends = over_m((8 - p) % 8, 0) if j2lo == 0 else over_m(7 - p, 1)
            return jnp.where(lane < 16, ends, over_m(7 - p, 1 - j2lo))

        own = lax.broadcasted_iota(jnp.int32, (16, 128), 0)

        def plane_of(plane):
            def load(p, jj):
                block = received(p, jj) if (p >= 4) == (plane == 1) else opposite_block(p, jj)
                if p % 4 == 0 and jj < 2:
                    low, high = received(p, jj), opposite_block(p, jj)
                    if plane == 1:
                        low, high = high, low
                    on = jnp.where(own < 8, low, high)
                    if jj == 0:
                        spot = jnp.logical_and(lane == 0, own == 8 * (1 - plane))
                        on = jnp.where(spot, n_recv[(p // 4) * 2 + 1 - plane, pl.ds(0, 1), :], on)
                    block = jnp.where(lane < 16, on, block)
                return block

            return load

        for plane in range(2):
            arrange(plane, plane_of(plane))

    send_forward(1, 0)
    send_forward(1, 1)
    for load in loads[3:]:
        load.wait()
    for j2a in range(4):
        for k in range(2):
            tables_back[j2a, k] = tables[T_C + j2a, k].astype(F32).T.astype(BF16)

    def send_back(f):
        for half in (1, 0):
            over_half(send(
                lambda d: b_send.at[f, block_of(d)], b_recv.at[f, block_of(me)],
                send_sems.at[6 + f], recv_sems.at[4 + f]), half)

    @pl.loop(0, 2)
    def _(f):
        finish(f_recv.at[f, pl.ds(0, 127 * 8)], recv_sems.at[2 + f])
        for part in range(2):
            values = jnp.concatenate([
                jnp.concatenate([
                    f_recv[f, pl.ds(ri * 4 + part * 2 + l, 128, stride=8), :] for l in range(2)], 1)
                for ri in range(2)], 0)
            high, low = split(values)
            y_mid[:, part * 256:(part + 1) * 256] = (
                dot(tables[T_P, 0], high) + dot(tables[T_P, 0], low) + dot(tables[T_P, 1], high))

        @pl.loop(0, 8)
        def _(n):
            at = pl.multiple_of(n * 16, 16)
            real, imag = [], []
            for l in range(4):
                lanes = slice(l * 128, (l + 1) * 128)
                vr, vi = y_mid[pl.ds(at, 16), lanes], y_mid[pl.ds(128 + at, 16), lanes]
                wr, wi = twiddle[0, pl.ds(at, 16), lanes], twiddle[1, pl.ds(at, 16), lanes]
                real.append(vr * wr - vi * wi)
                imag.append(vr * wi + vi * wr)
            r02, r13 = real[0] + real[2], real[1] + real[3]
            i02, i13 = imag[0] + imag[2], imag[1] + imag[3]
            rd, re = real[0] - real[2], real[1] - real[3]
            id_, ie = imag[0] - imag[2], imag[1] - imag[3]
            outs = ((r02 + r13, i02 + i13), (rd + ie, id_ - re), (r02 - r13, i02 - i13), (rd - ie, id_ + re))
            for j2a, pair in enumerate(outs):
                for ri in range(2):
                    high, low = split(pair[ri])
                    v_high[j2a, pl.ds(at, 16), ri * 128:(ri + 1) * 128] = high
                    v_low[j2a, pl.ds(at, 16), ri * 128:(ri + 1) * 128] = low

        for j2a in range(4):
            high, low = v_high[j2a], v_low[j2a]
            spectral = (dot(high, tables[T_C + j2a, 0]) + dot(low, tables[T_C + j2a, 0])
                        + dot(high, tables[T_C + j2a, 1]))
            factor = scale[jnp.where(me == 0, f, 0), j2a]
            high, low = split(spectral * jnp.concatenate([factor, factor], 1))
            v_back[j2a] = (dot(high, tables_back[j2a, 0]) + dot(low, tables_back[j2a, 0])
                           + dot(high, tables_back[j2a, 1]))

        @pl.loop(0, 8)
        def _(n):
            at = pl.multiple_of(n * 16, 16)
            real = [v_back[j2a, pl.ds(at, 16), 0:128] for j2a in range(4)]
            imag = [v_back[j2a, pl.ds(at, 16), 128:256] for j2a in range(4)]
            r02, r13 = real[0] + real[2], real[1] + real[3]
            i02, i13 = imag[0] + imag[2], imag[1] + imag[3]
            rd, re = real[0] - real[2], real[1] - real[3]
            id_, ie = imag[0] - imag[2], imag[1] - imag[3]
            outs = ((r02 + r13, i02 + i13), (rd - ie, id_ + re), (r02 - r13, i02 - i13), (rd + ie, id_ - re))
            for l, (vr, vi) in enumerate(outs):
                lanes = slice(l * 128, (l + 1) * 128)
                wr, wi = twiddle[0, pl.ds(at, 16), lanes], twiddle[1, pl.ds(at, 16), lanes]
                for ri, value in enumerate((vr * wr + vi * wi, vi * wr - vr * wi)):
                    high, low = split(value)
                    z_high[pl.ds(ri * 128 + at, 16), lanes] = high
                    z_low[pl.ds(ri * 128 + at, 16), lanes] = low

        for part in range(2):
            high, low = z_high[:, part * 256:(part + 1) * 256], z_low[:, part * 256:(part + 1) * 256]
            out = dot(tables[T_PI, 0], high) + dot(tables[T_PI, 0], low) + dot(tables[T_PI, 1], high)
            for ri in range(2):
                for l in range(2):
                    half, row = jnp.where(me == 0, ri, f), jnp.where(me == 0, f, ri)
                    b_send[half, pl.ds(row * 4 + part * 2 + l, 128, stride=8), :] = (
                        out[ri * 128:(ri + 1) * 128, l * 128:(l + 1) * 128])

        @pl.when(jnp.logical_and(me == 0, f == 1))
        def _():
            send_back(0)

        @pl.when(jnp.logical_or(me != 0, f == 1))
        def _():
            send_back(f)

    for f in range(2):
        b_recv[f, block_of(me), :] = b_send[f, block_of(me), :]

    def over_column(action):
        for dx in (2, 1, 3, 0):
            for dz in (1, 0):
                for dc in (1, 0):
                    if (dx, dz, dc) != (0, 0, 0):
                        action(lax.rem(x + dx, 4) * 4 + lax.rem(zl + dz, 2) * 2 + lax.rem(c + dc, 2))

    def send_pieces(f, phase, pairs_of_refs):
        over_column(lambda g: [pltpu.make_async_remote_copy(
            source.at[g], target.at[column], route_send_sems.at[phase + k, f], route_recv_sems.at[phase + k, f],
            device_id=line + g, device_id_type=LOGICAL).start()
            for k, (source, target) in enumerate(pairs_of_refs)])
        for source, target in pairs_of_refs:
            target[column] = source[column]

    def await_pieces(f, phase, pairs_of_refs):
        for k, (_, target) in enumerate(pairs_of_refs):
            finish(target.at[pl.ds(0, 15)], route_recv_sems.at[phase + k, f])

    first_refs = [((r_send.at[0], r_recv), (r_send_rest.at[0], r_recv_rest)),
                  ((r_send.at[1], r_other), (r_send_rest.at[1], r_other_rest))]
    second_refs = [((t_send.at[f], t_recv.at[f]), (t_send_rest.at[f], t_recv_rest.at[f])) for f in range(2)]

    fewer = lax.broadcasted_iota(jnp.int32, (32, 128), 1) < 64

    for f in range(2):
        finish(b_recv.at[f, pl.ds(0, 127 * 8)], recv_sems.at[4 + f])
        for l in range(4):
            cells = pl.ds(l * 128, 128)
            for ri in range(2):
                high, low = split(b_recv[f, pl.ds(ri * 4 + l, 128, stride=8), :].T)
                w_high[cells, ri * 128:(ri + 1) * 128] = high
                w_low[cells, ri * 128:(ri + 1) * 128] = low
        for part in range(2):
            cells = pl.ds(part * 256, 256)
            high, low = w_high[cells, :], w_low[cells, :]
            fields = dot(high, tables[T_U, 0]) + dot(low, tables[T_U, 0]) + dot(high, tables[T_U, 1])
            modulus = jnp.exp(0.5 * fields)
            modulus_ref[f, cells, :] = modulus
            high, low = split(modulus)
            high, low = split(dot(high, pairs[...]) + dot(low, pairs[...]))
            g_high[cells, :] = high
            g_low[cells, :] = low
        coarse = dot(rows[...], g_high[...]) + dot(rows[...], g_low[...])
        r_send[f] = coarse[0:128, 0:128].reshape(16, 8, 128)
        r_send_rest[f] = jnp.where(fewer, coarse[128:160, 128:256], coarse[160:192, 128:256]).reshape(16, 2, 128)
        send_pieces(f, 0, first_refs[f])

    for f in range(2):
        await_pieces(f, 0, first_refs[f])
        (_, held), (_, held_rest) = first_refs[f]

        @pl.loop(0, 16)
        def _(g):
            t_send[f, g] = held[order_smem[0, g]]
            second, third = held_rest[order_smem[1, g]], held_rest[order_smem[2, g]]
            t_send_rest[f, g] = jnp.where(fewer[0:2], second, third)

        send_pieces(f, 2, second_refs[f])

    for f in range(2):
        await_pieces(f, 2, second_refs[f])
        fine_ref[f] = t_recv[f]
        rest_ref[f] = t_recv_rest[f]

    finish(s_send.at[pl.ds(0, 127)], send_sems.at[0])

    @pl.when(extra)
    def _():
        finish(n_send.at[0], send_sems.at[1])

    for f in range(2):
        finish(b_send.at[f, pl.ds(0, 127 * 8)], send_sems.at[6 + f])
        for k, (whole, rest) in enumerate(((r_send, r_send_rest), (t_send, t_send_rest))):
            finish(whole.at[f, pl.ds(0, 15)], route_send_sems.at[2 * k, f])
            finish(rest.at[f, pl.ds(0, 15)], route_send_sems.at[2 * k + 1, f])
    for f in range(2):
        for half in range(2):
            forward_sent(f, half)


def finisher(modulus_ref, fine_ref, rest_ref, modulus_hbm, one_hbm, two_hbm, three_hbm, two, three, sems):
    stores = [
        pltpu.make_async_copy(source, target, sems.at[k]) for k, (source, target) in enumerate((
            (modulus_ref, modulus_hbm), (fine_ref, one_hbm), (two, two_hbm), (three, three_hbm)))]
    stores[0].start()
    stores[1].start()
    for f in range(2):
        rest = rest_ref[f]
        two[pl.ds(f * 32, 32), :] = rest.reshape(32, 128)[:, 0:64]
        three[pl.ds(f * 8, 8), :] = rest[0:8, 0, 64:96]
    stores[2].start()
    stores[3].start()
    for store in stores:
        store.wait()


def on_device(white_noise, spectrum, group_table):
    tables, twiddle, pairs, rows = build_tables()
    hbm = pl.BlockSpec(memory_space=pltpu.HBM)
    vmem = pl.BlockSpec(memory_space=pltpu.VMEM)
    modulus_shape = jax.ShapeDtypeStruct((2, CELLS, NZ), F32)
    modulus, fine, rest = pl.pallas_call(
        kernel,
        out_shape=(pltpu.VMEM((2, CELLS, NZ), F32), pltpu.VMEM((2, 16, 8, 128), F32), pltpu.VMEM((2, 16, 2, 128), F32)),
        in_specs=[hbm] * 7,
        out_specs=(vmem, vmem, vmem),
        scratch_shapes=[
            pltpu.SMEM((3, 16), jnp.int32),
            pltpu.VMEM((2, CELLS, NZ), F32),
            pltpu.VMEM((CELLS, NZ), F32),
            pltpu.VMEM((TABLES, 2, 256, 256), BF16),
            pltpu.VMEM((2, 128, CELLS), F32),
            pltpu.VMEM((NZ, 256), BF16),
            pltpu.VMEM((192, CELLS), BF16),
            pltpu.VMEM((4, 2, 256, 256), BF16),
            pltpu.VMEM((128, 4, 128), F32),
            pltpu.VMEM((128, 4, 128), F32),
            pltpu.VMEM((1, 4, 128), F32),
            pltpu.VMEM((4, 4, 128), F32),
            *[pltpu.VMEM((128, 4, 128), F32)] * 3,
            pltpu.VMEM((2, 4, 128, 128), F32),
            pltpu.VMEM((2, 1024, 128), F32),
            pltpu.VMEM((2, 1024, 128), F32),
            pltpu.VMEM((2, 1024, 128), F32),
            pltpu.VMEM((2, 1024, 128), F32),
            pltpu.VMEM((256, CELLS), F32),
            pltpu.VMEM((4, 128, 256), BF16),
            pltpu.VMEM((4, 128, 256), BF16),
            pltpu.VMEM((4, 128, 256), F32),
            pltpu.VMEM((256, CELLS), BF16),
            pltpu.VMEM((256, CELLS), BF16),
            *[pltpu.VMEM((CELLS, 256), BF16)] * 4,
            *[pltpu.VMEM((*count, 16, size, 128), F32) for size in (8, 2) for count in ((2,), (), ())],
            *[pltpu.VMEM((2, 16, size, 128), F32) for size in (8, 8, 2, 2)],
            pltpu.SemaphoreType.DMA((8,)),
            pltpu.SemaphoreType.DMA((8,)),
            pltpu.SemaphoreType.DMA((6,)),
            pltpu.SemaphoreType.DMA((4, 2)),
            pltpu.SemaphoreType.DMA((4, 2)),
        ],
        compiler_params=pltpu.CompilerParams(
            collective_id=0, has_side_effects=True, vmem_limit_bytes=60000000),
        name="moduli",
    )(
        white_noise.reshape(2, CELLS, NZ), spectrum.reshape(CELLS, NZ), group_table,
        jnp.asarray(tables), jnp.asarray(twiddle), jnp.asarray(pairs), jnp.asarray(rows),
    )
    modulus, one, two, three = pl.pallas_call(
        finisher,
        out_shape=(
            modulus_shape,
            jax.ShapeDtypeStruct((2, 16, 8, 128), F32),
            jax.ShapeDtypeStruct((64, 64), F32),
            jax.ShapeDtypeStruct((16, 32), F32),
        ),
        in_specs=[vmem, vmem, vmem],
        out_specs=(hbm, hbm, hbm, hbm),
        scratch_shapes=[pltpu.VMEM((64, 64), F32), pltpu.VMEM((16, 32), F32), pltpu.SemaphoreType.DMA((4,))],
        compiler_params=pltpu.CompilerParams(vmem_limit_bytes=4 << 20),
        name="levels",
    )(modulus, fine, rest)
    return (
        modulus.reshape(2, CX, CY, NZ),
        one.reshape(2, 8, 16, 128),
        two.reshape(2, 4, 8, 64),
        three.reshape(2, 2, 4, 32),
    )


def solution(mesh):
    split_mesh = Mesh(mesh.devices.reshape(2, 4, 4, 2, 2), (*PX, *PY))
    whole = P(None, PX, PY, None)
    return jax.shard_map(
        on_device,
        mesh=split_mesh,
        in_specs=(whole, P(PX, PY, None), P()),
        out_specs=(whole, whole, whole, whole),
        check_vma=False,
    )
```
